32 devices in a mesh: grp: 2 (over y), gx: 16 (over z, x, core), gy: 1.
Axes of the slice: x: 2, y: 2, z: 4, core: 2. Of those that a mesh axis runs over, the one named last changes fastest.
Arguments:
- residue_feats: bfloat16 [512, 256], P(('grp', 'gx')), parts along dimension 0, may hold values from -6 to 6
- pair_feats: bfloat16 [64, 512, 256], P(None, ('grp', 'gx'), 'gy'), parts along dimension 1, may hold values from -30 to 30
- w_row: bfloat16 [256, 64], replicated, may hold values from -0.375 to 0.375
- w_col: bfloat16 [256, 64], replicated, may hold values from -0.375 to 0.375
- first_taps: bfloat16 [9, 64, 64], replicated, may hold values from -0.25 to 0.25
- second_taps: bfloat16 [9, 64, 64], replicated, may hold values from -0.25 to 0.25
- norm_scale: float32 [2, 64], replicated, may hold values from 0.25 to 1.75
- norm_shift: float32 [2, 64], replicated, may hold values from -2 to 2
Outputs:
- symmetric: bfloat16 [64, 512, 256], P(None, ('grp', 'gx'), 'gy'), parts along dimension 1
The draws below stay inside these ranges and needn't reach their ends.
There are 2 independent parts, one for each index of `grp`. The reference program is written for one: setup_inputs(seed, part) draws one part's arguments, and reference() takes and returns one part's arrays. A program takes and returns all parts, laid end to end along the dimension named above; an argument that names none is the same for every part. Nothing has to cross between parts.
All inputs are finite; a program needn't handle non-finite values.
Results may differ from the reference program's by a relative error of at most 0.012.
Values may be sent and summed in bfloat16 or wider, within the bound.
A program may use at most 64 MiB of HBM per device.

```python
import math
import jax
import jax.numpy as jnp
from jax import lax

CH = 64
FEAT = 256
DILATION_STEP = 8
L = 256


def draw_pair_feats(key, part):
    key_noise = jax.random.fold_in(key, 11)
    key_rows = jax.random.fold_in(key, 12)
    key_cols = jax.random.fold_in(key, 13)
    key_level = jax.random.fold_in(key, 14)
    row_scale = jnp.exp(jax.random.uniform(key_rows, (L,), jnp.float32, 0.0, 0.5 * math.log(10.0)))
    col_scale = jnp.exp(jax.random.uniform(key_cols, (L,), jnp.float32, 0.0, 0.5 * math.log(10.0)))
    level = 0.5 * jax.random.truncated_normal(key_level, -3.0, 3.0, (CH, 1, 1), jnp.float32)
    position = jnp.arange(L, dtype=jnp.float32) / L
    noise = jax.random.truncated_normal(key_noise, -5.0, 5.0, (CH, L, L), jnp.float32)
    ramp = 0.5 + 1.5 * position
    value = noise * row_scale[None, :, None] * col_scale[None, None, :] / 3.0 + level * ramp[None, :, None]
    return value.astype(jnp.bfloat16)


def steps_of(own_key, shape, shards, smallest, largest):
    factor_of = 1.0
    for dim, shards_of in shards:
        heights = jax.random.uniform(jax.random.fold_in(jax.random.fold_in(own_key, 6), dim), (shards_of,), jnp.float32, smallest / len(shards), largest / len(shards))
        factor_of = factor_of * jnp.repeat(jnp.exp(heights), shape[dim] // shards_of).reshape((-1,) + (1,) * (len(shape) - 1 - dim))
    return factor_of


def normal_values(own_key, dims, scale, bound, split=(), kind=jnp.bfloat16):
    result = jax.random.normal(own_key, dims, jnp.float32) * scale
    if len(split) > 0:
        result = steps_of(own_key, dims, split, -0.22, 0.18) * result
    return jnp.clip(result, min=-bound, max=bound).astype(kind)


def setup_inputs(seed: int = 0, part: int = 0) -> dict:
    key_list = jax.random.split(jax.random.key(seed), 9)
    own_keys = jax.random.split(jax.random.fold_in(key_list[8], part), 9)
    residue_feats = normal_values(own_keys[0], (L, FEAT), 1.0, 6.0, ((0, 16),))
    pair_feats = draw_pair_feats(jax.random.fold_in(jax.random.fold_in(key_list[8], part), 71), part)
    w_row = normal_values(key_list[2], (FEAT, CH), FEAT ** -0.5, 0.375)
    w_col = normal_values(key_list[3], (FEAT, CH), FEAT ** -0.5, 0.375)
    first_taps = normal_values(key_list[4], (9, CH, CH), (9 * CH) ** -0.5, 0.25)
    second_taps = normal_values(key_list[5], (9, CH, CH), (9 * CH) ** -0.5, 0.25)
    norm_scale = jnp.clip(1.0 + 0.15 * jax.random.normal(key_list[6], (2, CH), jnp.float32), 0.25, 1.75)
    norm_shift = normal_values(key_list[7], (2, CH), 0.5, 2.0, (), jnp.float32)
    return {"residue_feats": residue_feats, "pair_feats": pair_feats, "w_row": w_row, "w_col": w_col, "first_taps": first_taps, "second_taps": second_taps, "norm_scale": norm_scale, "norm_shift": norm_shift}


epsilon = 1e-05

def dilated(receptive_region, weights):
    filter_weight = jnp.transpose(weights.reshape(3, 3, CH, CH), (2, 3, 0, 1))
    tap_sum_total = lax.conv_general_dilated(receptive_region[None], filter_weight, (1, 1), ((DILATION_STEP, DILATION_STEP), (DILATION_STEP, DILATION_STEP)), rhs_dilation=(DILATION_STEP, DILATION_STEP), dimension_numbers=('NCHW', 'OIHW', 'NCHW'), preferred_element_type=jnp.float32)
    return tap_sum_total[0]

def normalized(tap_sum_total, gain, shift):
    average = lax.optimization_barrier(jnp.mean(tap_sum_total, axis=(1, 2)))
    centred = tap_sum_total - average[:, None, None]
    spread = lax.optimization_barrier(jnp.mean(centred * centred, axis=(1, 2)))
    factor = gain * lax.rsqrt(spread + epsilon)
    return centred * factor[:, None, None] + shift[:, None, None]

def reference(residue_feats, pair_feats, w_row, w_col, first_taps, second_taps, norm_scale, norm_shift):
    row_part = jnp.dot(residue_feats, w_row, preferred_element_type=jnp.float32).astype(jnp.bfloat16)
    col_part = jnp.dot(residue_feats, w_col, preferred_element_type=jnp.float32).astype(jnp.bfloat16)
    block_in = (pair_feats.astype(jnp.float32) + row_part.T.astype(jnp.float32)[:, :, None] + col_part.T.astype(jnp.float32)[:, None, :]).astype(jnp.bfloat16)
    first_conv = dilated(block_in, first_taps)
    activated = jax.nn.elu(normalized(first_conv, norm_scale[0], norm_shift[0])).astype(jnp.bfloat16)
    second_conv = dilated(activated, second_taps)
    block_out = jax.nn.elu(block_in.astype(jnp.float32) + normalized(second_conv, norm_scale[1], norm_shift[1])).astype(jnp.bfloat16)
    mirrored = jnp.transpose(block_out, (0, 2, 1))
    return (0.5 * (block_out.astype(jnp.float32) + mirrored.astype(jnp.float32))).astype(jnp.bfloat16)
```

```python
import functools

import jax
import jax.numpy as jnp
from jax import lax
from jax.experimental import pallas as pl
from jax.experimental.pallas import tpu as pltpu
from jax.sharding import PartitionSpec as P

DILATION_STEP = 8


epsilon = 1e-05


def with_halo(cells, sides, width):
    for axis, dim in sides:
        count = lax.axis_size(axis)
        ends = count - 1
        head = lax.slice_in_dim(cells, 0, width, axis=dim)
        tail = lax.slice_in_dim(cells, cells.shape[dim] - width, cells.shape[dim], axis=dim)
        cells = jnp.concatenate(
            [
                lax.ppermute(tail, axis, [(i, (i + 1) % count) for i in range(ends)]),
                cells,
                lax.ppermute(head, axis, [((i + 1) % count, i) for i in range(ends)]),
            ],
            axis=dim,
        )
    return cells


def dilated(receptive_region, weights):
    row_count = receptive_region.shape[1]
    col_count = receptive_region.shape[2]
    border_padded_input = with_halo(receptive_region, (("gx", 1), ("gy", 2)), DILATION_STEP)
    tap_sum_total = jnp.zeros((weights.shape[1], row_count, col_count), jnp.float32)
    for filter_tap_index in range(9):
        row_displacement = filter_tap_index // 3 * DILATION_STEP
        column_displacement = filter_tap_index % 3 * DILATION_STEP
        window = border_padded_input[
            :,
            row_displacement : row_displacement + row_count,
            column_displacement : column_displacement + col_count,
        ]
        tap_sum_total = tap_sum_total + jnp.einsum(
            "oc,crw->orw", weights[filter_tap_index], window, preferred_element_type=jnp.float32
        )
    return tap_sum_total


def normalized(tap_sum_total, gain, shift):
    cell_count = (
        tap_sum_total.shape[1] * tap_sum_total.shape[2] * lax.axis_size("gx") * lax.axis_size("gy")
    )
    first_sum, second_sum = lax.psum(
        (jnp.sum(tap_sum_total, axis=(1, 2)), jnp.sum(tap_sum_total * tap_sum_total, axis=(1, 2))),
        ("gx", "gy"),
    )
    average = first_sum / cell_count
    spread = second_sum / cell_count - average * average
    centred = tap_sum_total - average[:, None, None]
    factor = gain * lax.rsqrt(spread + epsilon)
    return centred * factor[:, None, None] + shift[:, None, None]


def body(residue_feats, pair_feats, w_row, w_col, first_taps, second_taps, norm_scale, norm_shift):
    col_count = pair_feats.shape[2]
    col_start = lax.axis_index("gy") * col_count
    row_part = jnp.dot(residue_feats, w_row, preferred_element_type=jnp.float32).astype(
        jnp.bfloat16
    )
    everyone = lax.all_gather(residue_feats, "gx", axis=0, tiled=True)
    col_feats = lax.dynamic_slice_in_dim(everyone, col_start, col_count, 0)
    col_part = jnp.dot(col_feats, w_col, preferred_element_type=jnp.float32).astype(jnp.bfloat16)
    block_in = (
        pair_feats.astype(jnp.float32)
        + row_part.T.astype(jnp.float32)[:, :, None]
        + col_part.T.astype(jnp.float32)[:, None, :]
    ).astype(jnp.bfloat16)
    first_conv = dilated(block_in, first_taps)
    activated = jax.nn.elu(normalized(first_conv, norm_scale[0], norm_shift[0])).astype(
        jnp.bfloat16
    )
    second_conv = dilated(activated, second_taps)
    block_out = jax.nn.elu(
        block_in.astype(jnp.float32) + normalized(second_conv, norm_scale[1], norm_shift[1])
    ).astype(jnp.bfloat16)
    whole_rows = lax.all_gather(block_out, "gy", axis=2, tiled=True)
    columns = lax.all_to_all(whole_rows, "gx", split_axis=2, concat_axis=1, tiled=True)
    flipped = lax.dynamic_slice_in_dim(columns, col_start, col_count, 1)
    mirrored = jnp.transpose(flipped, (0, 2, 1))
    return (0.5 * (block_out.astype(jnp.float32) + mirrored.astype(jnp.float32))).astype(
        jnp.bfloat16
    )


MESH = pl.DeviceIdType.MESH
D = DILATION_STEP
BF = jnp.bfloat16
F32 = jnp.float32


def low_half():
    return lax.broadcasted_iota(jnp.int32, (1, 128), 1) < 64


def half_roll(v):
    return pltpu.roll(v, 64, 1)


def three_shifts(v):
    gap = jnp.zeros((D, v.shape[1]), v.dtype)
    left = jnp.concatenate([gap, v[:-D]], axis=0)
    right = jnp.concatenate([v[D:], gap], axis=0)
    return jnp.concatenate([left.astype(BF), v.astype(BF), right.astype(BF)], axis=1)


def times(a, w):
    return lax.dot_general(a, w, (((1,), (1,)), ((), ())), preferred_element_type=F32)


def fold_rows(v):
    return jnp.sum(v.reshape(v.shape[0] // 8, 8, v.shape[1]), axis=0)


def elu(v):
    return jnp.where(v > 0, v, jnp.exp(jnp.minimum(v, 0.0)) - 1.0)


def fused(
    n,
    pair_hbm, feats, w_row, w_col, taps1, taps2, scale, shift,
    out,
    pair_v, p32, halo_up, halo_dn, h32, all_feats, own_w, halo_w,
    shifts, acc, send_up, send_dn, got_up, got_dn, stats, block, mirror, m32,
    in_sem, feat_s, feat_r, halo_s, halo_r, stat_s, stat_r, edge_s, edge_r, mir_s, mir_r,
):
    me = lax.axis_index("gx")
    cols = pair_v.shape[2]
    cells = float(n * 2 * D * cols)
    rows = 2 * D
    ch = pair_v.shape[0]
    low = low_half()

    barrier = pltpu.get_barrier_semaphore()

    @pl.loop(1, n)
    def _(k):
        pl.semaphore_signal(
            barrier, inc=1, device_id={"gx": lax.rem(me + k, n)}, device_id_type=MESH
        )

    load = pltpu.make_async_copy(pair_hbm, pair_v, in_sem)
    load.start()

    for index, taps in enumerate((taps1, taps2)):
        t = taps[...].astype(F32)
        none = jnp.zeros_like(t[0])
        for kx in range(3):
            where = slice(kx * 128, kx * 128 + 128)
            top = jnp.concatenate([t[3 + kx], t[6 + kx]], axis=1)
            bottom = jnp.concatenate([t[kx], t[3 + kx]], axis=1)
            own_w[index, :, where] = jnp.concatenate([top, bottom], axis=0).astype(BF)
            top = jnp.concatenate([t[kx], none], axis=1)
            bottom = jnp.concatenate([none, t[6 + kx]], axis=1)
            halo_w[index, :, where] = jnp.concatenate([top, bottom], axis=0).astype(BF)

    pl.semaphore_wait(barrier, n - 1)

    def copy_to(src, dst, s, r, peer):
        return pltpu.make_async_remote_copy(
            src_ref=src, dst_ref=dst, send_sem=s, recv_sem=r,
            device_id={"gx": peer}, device_id_type=MESH,
        )

    above = jnp.maximum(me - 1, 0)
    below = jnp.minimum(me + 1, n - 1)
    up1 = copy_to(pair_hbm.at[:, pl.ds(0, D), :], halo_dn, halo_s.at[0], halo_r.at[0], above)
    dn1 = copy_to(pair_hbm.at[:, pl.ds(D, D), :], halo_up, halo_s.at[1], halo_r.at[1], below)

    def feat_copy(k):
        return copy_to(
            feats, all_feats.at[me], feat_s.at[k], feat_r.at[k], lax.rem(me + k, n)
        )

    def stat_copy(index, k):
        return copy_to(
            stats.at[index, me], stats.at[index, me], stat_s.at[index, k], stat_r.at[index, k],
            lax.rem(me + k, n),
        )

    def mirror_copy(k):
        peer = lax.rem(me + k, n)
        start = pl.multiple_of(peer * rows, rows)
        return copy_to(
            block.at[:, pl.ds(start, rows), :], mirror.at[me], mir_s.at[k], mir_r.at[k], peer
        )

    def edges_start(first, second):
        @pl.when(me > 0)
        def _():
            first.start()

        @pl.when(me < n - 1)
        def _():
            second.start()

    def edges_wait_recv(first, second):
        @pl.when(me < n - 1)
        def _():
            first.wait_recv()

        @pl.when(me > 0)
        def _():
            second.wait_recv()

    def edges_wait_send(first, second):
        @pl.when(me > 0)
        def _():
            first.wait_send()

        @pl.when(me < n - 1)
        def _():
            second.wait_send()

    @pl.loop(1, n)
    def _(k):
        feat_copy(k).start()

    edges_start(up1, dn1)

    all_feats[me] = feats[...]
    load.wait()
    for h in range(cols // 128):
        part = pair_v[:, :, h * 128 : h * 128 + 128].astype(F32)
        p32[h] = part.reshape(ch * rows, 128)

    w_row2 = jnp.concatenate([w_row[...].astype(F32)] * 2, axis=1).astype(BF)
    w_col2 = jnp.concatenate([w_col[...].astype(F32)] * 2, axis=1).astype(BF)

    def rounded(a, w):
        return jnp.dot(a, w, preferred_element_type=F32).astype(BF).astype(F32)

    own_rows = rounded(feats[...], w_row2)
    own_rows = jnp.where(low, own_rows[:D], own_rows[D:])

    @pl.loop(1, n)
    def _(k):
        feat_copy(k).wait_recv()

    col_part = rounded(all_feats[...].reshape(n * rows, feats.shape[1]), w_col2)
    rows_up = rounded(all_feats[above], w_row2)[D:]
    rows_dn = rounded(all_feats[below], w_row2)[:D]
    halo_rows = jnp.where(low, rows_up, rows_dn)
    inside = jnp.where(low, (me > 0).astype(F32), (me < n - 1).astype(F32)) > 0.5

    def pick(values, i):
        chosen = lax.broadcasted_iota(jnp.int32, values.shape, 0) == i
        return jnp.sum(jnp.where(chosen, values, 0.0), axis=0, keepdims=True)

    @pl.loop(0, D)
    def _(i):
        halves = []
        for h in range(cols // 128):
            first = p32[h, pl.ds(i, ch, stride=rows), :]
            second = p32[h, pl.ds(i + D, ch, stride=rows), :]
            halves.append(jnp.concatenate([first, second], axis=0).T)
        v = jnp.concatenate(halves, axis=0) + pick(own_rows, i) + col_part
        v = v.astype(BF).astype(F32)
        moved = three_shifts(v)
        block[i] = v.astype(BF)
        acc[i] = times(moved, own_w[0])

    edges_wait_recv(up1, dn1)
    for h in range(cols // 128):
        where = slice(h * 128, h * 128 + 128)
        h32[0, h] = halo_up[:, :, where].astype(F32).reshape(ch * D, 128)
        h32[1, h] = halo_dn[:, :, where].astype(F32).reshape(ch * D, 128)

    zeros = jnp.zeros((8, 128), F32)

    def first_edge(i, sums):
        halves = []
        for h in range(cols // 128):
            first = h32[0, h, pl.ds(i, ch, stride=D), :]
            second = h32[1, h, pl.ds(i, ch, stride=D), :]
            halves.append(jnp.concatenate([first, second], axis=0).T)
        v = jnp.concatenate(halves, axis=0) + pick(halo_rows, i) + col_part
        v = jnp.where(inside, v, 0.0)
        a = acc[i] + times(three_shifts(v), halo_w[0])
        acc[i] = a
        return sums[0] + fold_rows(a), sums[1] + fold_rows(a * a)

    def publish(index, sums):
        lines = []
        for v in sums:
            v = jnp.sum(v, axis=0, keepdims=True)
            lines.append(v + half_roll(v))
        stats[index, me] = jnp.concatenate(lines + [jnp.zeros((6, 128), F32)], axis=0)

        @pl.loop(1, n)
        def _(k):
            stat_copy(index, k).start()

    def collect(index):
        @pl.loop(1, n)
        def _(k):
            stat_copy(index, k).wait_recv()

        total = jnp.sum(stats[index], axis=0)
        average = total[0:1] / cells
        spread = total[1:2] / cells - average * average
        gain = jnp.concatenate([scale[index : index + 1, :]] * 2, axis=1)
        base = jnp.concatenate([shift[index : index + 1, :]] * 2, axis=1)
        return average, gain * lax.rsqrt(spread + epsilon), base

    sums = lax.fori_loop(0, D, first_edge, (zeros, zeros))
    publish(0, sums)

    @pl.loop(0, D // 2)
    def _(i):
        early, late = acc[i], acc[i + D // 2]
        send_up[i] = jnp.where(low, early, half_roll(late)).astype(BF)
        send_dn[i] = jnp.where(low, half_roll(early), late).astype(BF)

    up2 = copy_to(send_up, got_dn, edge_s.at[0], edge_r.at[0], above)
    dn2 = copy_to(send_dn, got_up, edge_s.at[1], edge_r.at[1], below)
    edges_start(up2, dn2)

    average, factor, base = collect(0)

    @pl.loop(0, D)
    def _(i):
        a = elu((acc[i] - average) * factor + base)
        acc[i] = times(three_shifts(a), own_w[1])

    edges_wait_recv(up2, dn2)

    def second_edge(i, sums):
        u = got_up[i].astype(F32)
        d = got_dn[i].astype(F32)
        early = jnp.where(low, u, half_roll(d))
        late = jnp.where(low, half_roll(u), d)
        for offset, v in ((0, early), (D // 2, late)):
            v = jnp.where(inside, elu((v - average) * factor + base), 0.0)
            a = acc[i + offset] + times(three_shifts(v), halo_w[1])
            acc[i + offset] = a
            sums = sums[0] + fold_rows(a), sums[1] + fold_rows(a * a)
        return sums

    sums = lax.fori_loop(0, D // 2, second_edge, (zeros, zeros))
    publish(1, sums)
    average, factor, base = collect(1)

    @pl.loop(0, D)
    def _(i):
        v = block[i].astype(F32) + (acc[i] - average) * factor + base
        block[i] = elu(v).astype(BF)

    @pl.loop(1, n)
    def _(k):
        mirror_copy(k).start()

    mirror[me] = block[:, pl.ds(pl.multiple_of(me * rows, rows), rows), :]

    @pl.loop(1, n)
    def _(k):
        mirror_copy(k).wait_recv()

    @pl.loop(0, n)
    def _(e):
        start = pl.multiple_of(e * (D * rows), D * rows)
        m32[pl.ds(start, D * rows), :] = mirror[e].astype(F32).reshape(D * rows, 128)

    @pl.loop(0, D)
    def _(i):
        first = m32[pl.ds(i, n * D, stride=rows), :]
        second = m32[pl.ds(i + D, n * D, stride=rows), :]
        even = jnp.where(low, first, half_roll(second)).reshape(n, 1, D, 128)
        odd = jnp.where(low, half_roll(first), second).reshape(n, 1, D, 128)
        m = jnp.concatenate([even, odd], axis=1).reshape(cols, 128)
        v = 0.5 * (block[i].astype(F32) + m)
        for h in range(cols // 128):
            t = v[h * 128 : h * 128 + 128].T
            p32[h, pl.ds(i, ch, stride=rows), :] = t[:ch]
            p32[h, pl.ds(i + D, ch, stride=rows), :] = t[ch:]

    for h in range(cols // 128):
        out[:, :, h * 128 : h * 128 + 128] = p32[h].reshape(ch, rows, 128).astype(BF)

    @pl.loop(1, n)
    def _(k):
        feat_copy(k).wait_send()
        stat_copy(0, k).wait_send()
        stat_copy(1, k).wait_send()
        mirror_copy(k).wait_send()

    edges_wait_send(up1, dn1)
    edges_wait_send(up2, dn2)


def fused_body(n, *args):
    residue_feats, pair_feats = args[:2]
    ch, rows, cols = pair_feats.shape
    halves = cols // 128
    vmem = pl.BlockSpec(memory_space=pltpu.VMEM)
    dma = pltpu.SemaphoreType.DMA
    return pl.pallas_call(
        functools.partial(fused, n),
        out_shape=jax.ShapeDtypeStruct(pair_feats.shape, BF),
        in_specs=[pl.BlockSpec(memory_space=pl.ANY)] + [vmem] * 7,
        out_specs=vmem,
        scratch_shapes=[
            pltpu.VMEM((ch, rows, cols), BF),
            pltpu.VMEM((halves, ch * rows, 128), F32),
            pltpu.VMEM((ch, D, cols), BF),
            pltpu.VMEM((ch, D, cols), BF),
            pltpu.VMEM((2, halves, ch * D, 128), F32),
            pltpu.VMEM((n,) + residue_feats.shape, BF),
            pltpu.VMEM((2, 128, 384), BF),
            pltpu.VMEM((2, 128, 384), BF),
            pltpu.VMEM((8, 128), F32),
            pltpu.VMEM((D, cols, 128), F32),
            pltpu.VMEM((D // 2, cols, 128), BF),
            pltpu.VMEM((D // 2, cols, 128), BF),
            pltpu.VMEM((D // 2, cols, 128), BF),
            pltpu.VMEM((D // 2, cols, 128), BF),
            pltpu.VMEM((2, n, 8, 128), F32),
            pltpu.VMEM((D, cols, 128), BF),
            pltpu.VMEM((n, D, rows, 128), BF),
            pltpu.VMEM((n * D * rows, 128), F32),
            dma,
            dma((n,)), dma((n,)), dma((2,)), dma((2,)), dma((2, n)), dma((2, n)),
            dma((2,)), dma((2,)), dma((n,)), dma((n,)),
        ],
        compiler_params=pltpu.CompilerParams(
            collective_id=0, has_side_effects=True, vmem_limit_bytes=40 * 1024 * 1024
        ),
    )(pair_feats, residue_feats, *args[2:])


def solution(mesh):
    placed = (P(("grp", "gx"), None), P(None, ("grp", "gx"), "gy"), P(), P(), P(), P(), P(), P())
    n = mesh.shape["gx"]

    def chosen(*args):
        ch, rows, cols = args[1].shape
        fits = mesh.shape["gy"] == 1 and rows == 2 * D and cols == n * rows
        if fits and ch == 64 and cols % 128 == 0 and cols <= 512:
            return fused_body(n, *args)
        return body(*args)

    return jax.shard_map(
        chosen, mesh=mesh, in_specs=placed, out_specs=P(None, ("grp", "gx"), "gy"), check_vma=False
    )
```

```python
import functools

import jax
import jax.numpy as jnp
from jax import lax
from jax.experimental import pallas as pl
from jax.experimental.pallas import tpu as pltpu
from jax.sharding import PartitionSpec as P

DILATION_STEP = 8


epsilon = 1e-05


def with_halo(cells, sides, width):
    for axis, dim in sides:
        count = lax.axis_size(axis)
        ends = count - 1
        head = lax.slice_in_dim(cells, 0, width, axis=dim)
        tail = lax.slice_in_dim(cells, cells.shape[dim] - width, cells.shape[dim], axis=dim)
        cells = jnp.concatenate(
            [
                lax.ppermute(tail, axis, [(i, (i + 1) % count) for i in range(ends)]),
                cells,
                lax.ppermute(head, axis, [((i + 1) % count, i) for i in range(ends)]),
            ],
            axis=dim,
        )
    return cells


def dilated(receptive_region, weights):
    row_count = receptive_region.shape[1]
    col_count = receptive_region.shape[2]
    border_padded_input = with_halo(receptive_region, (("gx", 1), ("gy", 2)), DILATION_STEP)
    tap_sum_total = jnp.zeros((weights.shape[1], row_count, col_count), jnp.float32)
    for filter_tap_index in range(9):
        row_displacement = filter_tap_index // 3 * DILATION_STEP
        column_displacement = filter_tap_index % 3 * DILATION_STEP
        window = border_padded_input[
            :,
            row_displacement : row_displacement + row_count,
            column_displacement : column_displacement + col_count,
        ]
        tap_sum_total = tap_sum_total + jnp.einsum(
            "oc,crw->orw", weights[filter_tap_index], window, preferred_element_type=jnp.float32
        )
    return tap_sum_total


def normalized(tap_sum_total, gain, shift):
    cell_count = (
        tap_sum_total.shape[1] * tap_sum_total.shape[2] * lax.axis_size("gx") * lax.axis_size("gy")
    )
    first_sum, second_sum = lax.psum(
        (jnp.sum(tap_sum_total, axis=(1, 2)), jnp.sum(tap_sum_total * tap_sum_total, axis=(1, 2))),
        ("gx", "gy"),
    )
    average = first_sum / cell_count
    spread = second_sum / cell_count - average * average
    centred = tap_sum_total - average[:, None, None]
    factor = gain * lax.rsqrt(spread + epsilon)
    return centred * factor[:, None, None] + shift[:, None, None]


def body(residue_feats, pair_feats, w_row, w_col, first_taps, second_taps, norm_scale, norm_shift):
    col_count = pair_feats.shape[2]
    col_start = lax.axis_index("gy") * col_count
    row_part = jnp.dot(residue_feats, w_row, preferred_element_type=jnp.float32).astype(
        jnp.bfloat16
    )
    everyone = lax.all_gather(residue_feats, "gx", axis=0, tiled=True)
    col_feats = lax.dynamic_slice_in_dim(everyone, col_start, col_count, 0)
    col_part = jnp.dot(col_feats, w_col, preferred_element_type=jnp.float32).astype(jnp.bfloat16)
    block_in = (
        pair_feats.astype(jnp.float32)
        + row_part.T.astype(jnp.float32)[:, :, None]
        + col_part.T.astype(jnp.float32)[:, None, :]
    ).astype(jnp.bfloat16)
    first_conv = dilated(block_in, first_taps)
    activated = jax.nn.elu(normalized(first_conv, norm_scale[0], norm_shift[0])).astype(
        jnp.bfloat16
    )
    second_conv = dilated(activated, second_taps)
    block_out = jax.nn.elu(
        block_in.astype(jnp.float32) + normalized(second_conv, norm_scale[1], norm_shift[1])
    ).astype(jnp.bfloat16)
    whole_rows = lax.all_gather(block_out, "gy", axis=2, tiled=True)
    columns = lax.all_to_all(whole_rows, "gx", split_axis=2, concat_axis=1, tiled=True)
    flipped = lax.dynamic_slice_in_dim(columns, col_start, col_count, 1)
    mirrored = jnp.transpose(flipped, (0, 2, 1))
    return (0.5 * (block_out.astype(jnp.float32) + mirrored.astype(jnp.float32))).astype(
        jnp.bfloat16
    )


MESH = pl.DeviceIdType.MESH
D = DILATION_STEP
BF = jnp.bfloat16
F32 = jnp.float32


def low_half():
    return lax.broadcasted_iota(jnp.int32, (1, 128), 1) < 64


def half_roll(v):
    return pltpu.roll(v, 64, 1)


def three_shifts(v):
    gap = jnp.zeros((D, v.shape[1]), v.dtype)
    left = jnp.concatenate([gap, v[:-D]], axis=0)
    right = jnp.concatenate([v[D:], gap], axis=0)
    return jnp.concatenate([left.astype(BF), v.astype(BF), right.astype(BF)], axis=1)


def times(a, w):
    return lax.dot_general(a, w, (((1,), (1,)), ((), ())), preferred_element_type=F32)


def fold_rows(v):
    return jnp.sum(v.reshape(v.shape[0] // 8, 8, v.shape[1]), axis=0)


def elu(v):
    return jnp.where(v > 0, v, jnp.exp(jnp.minimum(v, 0.0)) - 1.0)


def fused(
    n,
    pair_hbm, feats_hbm, w_row_hbm, w_col_hbm, taps1_hbm, taps2_hbm, scale_hbm, shift_hbm,
    out,
    feats, w_row, w_col, taps1, taps2, scale, shift,
    pair, p32, all_feats, own_w, halo_w, col_conv, col_base, acc,
    edges, stats, block, mirror, m32, out_v,
    in_sem, feat_s, feat_r, stat_s, stat_r, edge_s, edge_r, mir_s, mir_r, out_sem,
):
    me = lax.axis_index("gx")
    ch, rows, cols = pair.shape
    half = n // 2
    side = lax.div(me, half)
    lane = lax.rem(me, half)
    cells = float(n * rows * cols)
    low = low_half()

    def peer_of(k):
        return lax.rem(side + 1 + lax.div(k, half), 2) * half + lax.rem(lane + k, half)

    def sender_of(k):
        return lax.rem(side + 1 + lax.div(k, half), 2) * half + lax.rem(lane + n - k, half)

    def far_peers(act):
        pl.loop(0, half)(act)

    def near_peers(act):
        pl.loop(half + 1, n)(act)

    def all_peers(act):
        far_peers(act)
        near_peers(act)

    barrier = pltpu.get_barrier_semaphore()

    @all_peers
    def _(k):
        pl.semaphore_signal(barrier, inc=1, device_id={"gx": peer_of(k)}, device_id_type=MESH)

    loads = [
        pltpu.make_async_copy(src, dst, in_sem.at[k])
        for k, (src, dst) in enumerate(
            (
                (feats_hbm, feats), (w_row_hbm, w_row), (pair_hbm, pair), (w_col_hbm, w_col),
                (taps1_hbm, taps1), (taps2_hbm, taps2), (scale_hbm, scale), (shift_hbm, shift),
            )
        )
    ]
    for load in loads:
        load.start()
    for load in loads:
        load.wait()

    def rounded(a, w):
        return times(a, w).astype(BF).astype(F32)

    w_row2 = jnp.concatenate([w_row[...]] * 2, axis=0)
    w_col2 = jnp.concatenate([w_col[...]] * 2, axis=0)
    own_rows = rounded(feats[...], w_row2)
    own_rows = jnp.where(low, own_rows[:D], own_rows[D:])
    halves = cols // 128
    for h in range(halves):
        part = pair[:, :, h * 128 : h * 128 + 128].astype(F32)
        p32[h] = part.reshape(ch * rows, 128)

    def pick(values, i):
        chosen = lax.broadcasted_iota(jnp.int32, values.shape, 0) == i
        return jnp.sum(jnp.where(chosen, values, 0.0), axis=0, keepdims=True)

    def with_rows(i):
        parts = []
        for h in range(halves):
            first = p32[h, pl.ds(i, ch, stride=rows), :]
            second = p32[h, pl.ds(i + D, ch, stride=rows), :]
            parts.append(jnp.concatenate([first, second], axis=0).T)
        return jnp.concatenate(parts, axis=0) + pick(own_rows, i)

    def pack(index, i, early, late):
        edges[index, 0, i] = jnp.where(low, early, half_roll(late)).astype(BF)
        edges[index, 1, i] = jnp.where(low, half_roll(early), late).astype(BF)

    @pl.loop(0, D // 2)
    def _(i):
        early, late = with_rows(i), with_rows(i + D // 2)
        block[i] = early.astype(BF)
        block[i + D // 2] = late.astype(BF)
        pack(0, i, early, late)

    for index, taps in enumerate((taps1, taps2)):
        t = taps[...].astype(F32)
        none = jnp.zeros_like(t[0])
        for kx in range(3):
            where = slice(kx * 128, kx * 128 + 128)
            top = jnp.concatenate([t[3 + kx], t[6 + kx]], axis=1)
            bottom = jnp.concatenate([t[kx], t[3 + kx]], axis=1)
            own_w[index, :, where] = jnp.concatenate([top, bottom], axis=0).astype(BF)
            top = jnp.concatenate([t[kx], none], axis=1)
            bottom = jnp.concatenate([none, t[6 + kx]], axis=1)
            halo_w[index, :, where] = jnp.concatenate([top, bottom], axis=0).astype(BF)

    pl.semaphore_wait(barrier, n - 1)

    def copy_to(src, dst, s, r, peer):
        return pltpu.make_async_remote_copy(
            src_ref=src, dst_ref=dst, send_sem=s, recv_sem=r,
            device_id={"gx": peer}, device_id_type=MESH,
        )

    def feat_copy(k):
        return copy_to(feats, all_feats.at[me], feat_s.at[k], feat_r.at[k], peer_of(k))

    def stat_copy(index, k):
        return copy_to(
            stats.at[index, me], stats.at[index, me], stat_s.at[index, k], stat_r.at[index, k],
            peer_of(k),
        )

    def mirror_copy(k):
        peer = peer_of(k)
        start = pl.multiple_of(peer * rows, rows)
        return copy_to(
            block.at[:, pl.ds(start, rows), :], mirror.at[me], mir_s.at[k], mir_r.at[k], peer
        )

    def edge_copies(index):
        above, below = jnp.maximum(me - 1, 0), jnp.minimum(me + 1, n - 1)
        s, r = edge_s.at[index], edge_r.at[index]
        return (
            copy_to(edges.at[index, 0], edges.at[index, 3], s.at[0], r.at[0], above),
            copy_to(edges.at[index, 1], edges.at[index, 2], s.at[1], r.at[1], below),
        )

    def edges_start(index):
        first, second = edge_copies(index)

        @pl.when(me > 0)
        def _():
            first.start()

        @pl.when(me < n - 1)
        def _():
            second.start()

    def edges_wait_recv(index):
        first, second = edge_copies(index)

        @pl.when(me < n - 1)
        def _():
            first.wait_recv()

        @pl.when(me > 0)
        def _():
            second.wait_recv()

    def edges_wait_send(index):
        first, second = edge_copies(index)

        @pl.when(me > 0)
        def _():
            first.wait_send()

        @pl.when(me < n - 1)
        def _():
            second.wait_send()

    @all_peers
    def _(k):
        feat_copy(k).start()

    edges_start(0)
    all_feats[me] = feats[...]

    @pl.loop(0, D)
    def _(i):
        acc[i] = times(three_shifts(block[i].astype(F32)), own_w[0])

    @all_peers
    def _(k):
        feat_copy(k).wait_recv()

    inside = jnp.where(low, (me > 0).astype(F32), (me < n - 1).astype(F32)) > 0.5
    col_part = rounded(all_feats[...].reshape(n * rows, feats.shape[1]), w_col2)
    col_conv[...] = times(three_shifts(col_part), own_w[0]) + times(
        three_shifts(jnp.where(inside, col_part, 0.0)), halo_w[0]
    )
    col_base[...] = col_part + jnp.concatenate([shift[1:2, :]] * 2, axis=1)

    def unpacked(index, i):
        u = edges[index, 2, i].astype(F32)
        d = edges[index, 3, i].astype(F32)
        return jnp.where(low, u, half_roll(d)), jnp.where(low, half_roll(u), d)

    def add_sums(sums, a):
        return sums[0] + fold_rows(a), sums[1] + fold_rows(a * a)

    zeros = jnp.zeros((8, 128), F32)

    def publish(index, sums):
        lines = []
        for v in sums:
            v = jnp.sum(v, axis=0, keepdims=True)
            lines.append(v + half_roll(v))
        stats[index, me] = jnp.concatenate(lines + [jnp.zeros((6, 128), F32)], axis=0)

        @all_peers
        def _(k):
            stat_copy(index, k).start()

    def collect(index):
        @all_peers
        def _(k):
            stat_copy(index, k).wait_recv()

        total = jnp.sum(stats[index], axis=0)
        average = total[0:1] / cells
        spread = total[1:2] / cells - average * average
        gain = jnp.concatenate([scale[index : index + 1, :]] * 2, axis=1)
        return average, gain * lax.rsqrt(spread + epsilon)

    edges_wait_recv(0)

    def first_edge(i, sums):
        results = []
        for offset, v in zip((0, D // 2), unpacked(0, i)):
            v = jnp.where(inside, v, 0.0)
            a = acc[i + offset] + times(three_shifts(v), halo_w[0]) + col_conv[...]
            acc[i + offset] = a
            sums = add_sums(sums, a)
            results.append(a)
        pack(1, i, *results)
        return sums

    sums = lax.fori_loop(0, D // 2, first_edge, (zeros, zeros))
    publish(0, sums)
    edges_start(1)
    average, factor = collect(0)
    base = jnp.concatenate([shift[0:1, :]] * 2, axis=1)

    @pl.loop(0, D)
    def _(i):
        a = elu((acc[i] - average) * factor + base)
        acc[i] = times(three_shifts(a), own_w[1])

    edges_wait_recv(1)

    def second_edge(i, sums):
        for offset, v in zip((0, D // 2), unpacked(1, i)):
            v = jnp.where(inside, elu((v - average) * factor + base), 0.0)
            a = acc[i + offset] + times(three_shifts(v), halo_w[1])
            acc[i + offset] = a
            sums = add_sums(sums, a)
        return sums

    sums = lax.fori_loop(0, D // 2, second_edge, (zeros, zeros))
    publish(1, sums)
    average2, factor2 = collect(1)

    def result_of(which):
        where = pl.ds(pl.multiple_of(which * 128, 128), 128)

        @pl.loop(0, D)
        def _(i):
            v = block[i, where, :].astype(F32) + col_base[where, :]
            v = v + (acc[i, where, :] - average2) * factor2
            block[i, where, :] = elu(v).astype(BF)

    def widen(e):
        start = pl.multiple_of(e * (D * rows), D * rows)
        m32[pl.ds(start, D * rows), :] = mirror[e].astype(F32).reshape(D * rows, 128)

    def finish(which):
        where = pl.ds(pl.multiple_of(which * 128, 128), 128)
        offset = which * (half * D * rows)

        @pl.loop(0, D)
        def _(i):
            first = m32[pl.ds(offset + i, half * D, stride=rows), :]
            second = m32[pl.ds(offset + i + D, half * D, stride=rows), :]
            even = jnp.where(low, first, half_roll(second)).reshape(half, 1, D, 128)
            odd = jnp.where(low, half_roll(first), second).reshape(half, 1, D, 128)
            m = jnp.concatenate([even, odd], axis=1).reshape(128, 128)
            t = (0.5 * (block[i, where, :].astype(F32) + m)).T
            p32[which, pl.ds(i, ch, stride=rows), :] = t[:ch]
            p32[which, pl.ds(i + D, ch, stride=rows), :] = t[ch:]

        out_v[which] = p32[which].reshape(ch, rows, 128).astype(BF)
        copy = pltpu.make_async_copy(out_v.at[which], out.at[:, :, where], out_sem.at[which])
        copy.start()
        return copy

    result_of(1 - side)

    @far_peers
    def _(k):
        mirror_copy(k).start()

    result_of(side)

    @near_peers
    def _(k):
        mirror_copy(k).start()

    mirror[me] = block[:, pl.ds(pl.multiple_of(me * rows, rows), rows), :]
    widen(me)

    @near_peers
    def _(k):
        mirror_copy(k).wait_recv()
        widen(sender_of(k))

    near = finish(side)

    @all_peers
    def _(k):
        feat_copy(k).wait_send()
        stat_copy(0, k).wait_send()
        stat_copy(1, k).wait_send()

    edges_wait_send(0)
    edges_wait_send(1)

    @far_peers
    def _(k):
        mirror_copy(k).wait_recv()
        widen(sender_of(k))

    far = finish(1 - side)

    @all_peers
    def _(k):
        mirror_copy(k).wait_send()

    near.wait()
    far.wait()


def fused_body(n, *args):
    residue_feats, pair_feats = args[:2]
    ch, rows, cols = pair_feats.shape
    halves = cols // 128
    rest = (args[2].T, args[3].T) + args[4:]
    dma = pltpu.SemaphoreType.DMA
    return pl.pallas_call(
        functools.partial(fused, n),
        out_shape=jax.ShapeDtypeStruct(pair_feats.shape, BF),
        in_specs=[pl.BlockSpec(memory_space=pltpu.HBM)] * 8,
        out_specs=pl.BlockSpec(memory_space=pl.ANY),
        scratch_shapes=[
            *[pltpu.VMEM(a.shape, a.dtype) for a in (residue_feats,) + rest],
            pltpu.VMEM((ch, rows, cols), BF),
            pltpu.VMEM((halves, ch * rows, 128), F32),
            pltpu.VMEM((n,) + residue_feats.shape, BF),
            pltpu.VMEM((2, 128, 384), BF),
            pltpu.VMEM((2, 128, 384), BF),
            pltpu.VMEM((cols, 128), F32),
            pltpu.VMEM((cols, 128), F32),
            pltpu.VMEM((D, cols, 128), F32),
            pltpu.VMEM((2, 4, D // 2, cols, 128), BF),
            pltpu.VMEM((2, n, 8, 128), F32),
            pltpu.VMEM((D, cols, 128), BF),
            pltpu.VMEM((n, D, rows, 128), BF),
            pltpu.VMEM((n * D * rows, 128), F32),
            pltpu.VMEM((halves, ch, rows, 128), BF),
            dma((8,)),
            dma((n,)), dma((n,)), dma((2, n)), dma((2, n)), dma((2, 2)), dma((2, 2)),
            dma((n,)), dma((n,)), dma((2,)),
        ],
        compiler_params=pltpu.CompilerParams(
            collective_id=0, has_side_effects=True, vmem_limit_bytes=63 * 1024 * 1024
        ),
    )(pair_feats, residue_feats, *rest)


def solution(mesh):
    placed = (P(("grp", "gx"), None), P(None, ("grp", "gx"), "gy"), P(), P(), P(), P(), P(), P())
    n = mesh.shape["gx"]

    def chosen(*args):
        ch, rows, cols = args[1].shape
        fits = mesh.shape["gy"] == 1 and rows == 2 * D and cols == n * rows
        if fits and ch == 64 and cols == 256:
            return fused_body(n, *args)
        return body(*args)

    return jax.shard_map(
        chosen, mesh=mesh, in_specs=placed, out_specs=P(None, ("grp", "gx"), "gy"), check_vma=False
    )
```

```python
import functools

import jax
import jax.numpy as jnp
from jax import lax
from jax.experimental import pallas as pl
from jax.experimental.pallas import tpu as pltpu
from jax.sharding import PartitionSpec as P

DILATION_STEP = 8


epsilon = 1e-05


def with_halo(cells, sides, width):
    for axis, dim in sides:
        count = lax.axis_size(axis)
        ends = count - 1
        head = lax.slice_in_dim(cells, 0, width, axis=dim)
        tail = lax.slice_in_dim(cells, cells.shape[dim] - width, cells.shape[dim], axis=dim)
        cells = jnp.concatenate(
            [
                lax.ppermute(tail, axis, [(i, (i + 1) % count) for i in range(ends)]),
                cells,
                lax.ppermute(head, axis, [((i + 1) % count, i) for i in range(ends)]),
            ],
            axis=dim,
        )
    return cells


def dilated(receptive_region, weights):
    row_count = receptive_region.shape[1]
    col_count = receptive_region.shape[2]
    border_padded_input = with_halo(receptive_region, (("gx", 1), ("gy", 2)), DILATION_STEP)
    tap_sum_total = jnp.zeros((weights.shape[1], row_count, col_count), jnp.float32)
    for filter_tap_index in range(9):
        row_displacement = filter_tap_index // 3 * DILATION_STEP
        column_displacement = filter_tap_index % 3 * DILATION_STEP
        window = border_padded_input[
            :,
            row_displacement : row_displacement + row_count,
            column_displacement : column_displacement + col_count,
        ]
        tap_sum_total = tap_sum_total + jnp.einsum(
            "oc,crw->orw", weights[filter_tap_index], window, preferred_element_type=jnp.float32
        )
    return tap_sum_total


def normalized(tap_sum_total, gain, shift):
    cell_count = (
        tap_sum_total.shape[1] * tap_sum_total.shape[2] * lax.axis_size("gx") * lax.axis_size("gy")
    )
    first_sum, second_sum = lax.psum(
        (jnp.sum(tap_sum_total, axis=(1, 2)), jnp.sum(tap_sum_total * tap_sum_total, axis=(1, 2))),
        ("gx", "gy"),
    )
    average = first_sum / cell_count
    spread = second_sum / cell_count - average * average
    centred = tap_sum_total - average[:, None, None]
    factor = gain * lax.rsqrt(spread + epsilon)
    return centred * factor[:, None, None] + shift[:, None, None]


def body(residue_feats, pair_feats, w_row, w_col, first_taps, second_taps, norm_scale, norm_shift):
    col_count = pair_feats.shape[2]
    col_start = lax.axis_index("gy") * col_count
    row_part = jnp.dot(residue_feats, w_row, preferred_element_type=jnp.float32).astype(
        jnp.bfloat16
    )
    everyone = lax.all_gather(residue_feats, "gx", axis=0, tiled=True)
    col_feats = lax.dynamic_slice_in_dim(everyone, col_start, col_count, 0)
    col_part = jnp.dot(col_feats, w_col, preferred_element_type=jnp.float32).astype(jnp.bfloat16)
    block_in = (
        pair_feats.astype(jnp.float32)
        + row_part.T.astype(jnp.float32)[:, :, None]
        + col_part.T.astype(jnp.float32)[:, None, :]
    ).astype(jnp.bfloat16)
    first_conv = dilated(block_in, first_taps)
    activated = jax.nn.elu(normalized(first_conv, norm_scale[0], norm_shift[0])).astype(
        jnp.bfloat16
    )
    second_conv = dilated(activated, second_taps)
    block_out = jax.nn.elu(
        block_in.astype(jnp.float32) + normalized(second_conv, norm_scale[1], norm_shift[1])
    ).astype(jnp.bfloat16)
    whole_rows = lax.all_gather(block_out, "gy", axis=2, tiled=True)
    columns = lax.all_to_all(whole_rows, "gx", split_axis=2, concat_axis=1, tiled=True)
    flipped = lax.dynamic_slice_in_dim(columns, col_start, col_count, 1)
    mirrored = jnp.transpose(flipped, (0, 2, 1))
    return (0.5 * (block_out.astype(jnp.float32) + mirrored.astype(jnp.float32))).astype(
        jnp.bfloat16
    )


MESH = pl.DeviceIdType.MESH
D = DILATION_STEP
BF = jnp.bfloat16
F32 = jnp.float32


def low_half():
    return lax.broadcasted_iota(jnp.int32, (1, 128), 1) < 64


def half_roll(v):
    return pltpu.roll(v, 64, 1)


def three_shifts(v):
    gap = jnp.zeros((D, v.shape[1]), v.dtype)
    left = jnp.concatenate([gap, v[:-D]], axis=0)
    right = jnp.concatenate([v[D:], gap], axis=0)
    return jnp.concatenate([left.astype(BF), v.astype(BF), right.astype(BF)], axis=1)


def times(a, w):
    return lax.dot_general(a, w, (((1,), (1,)), ((), ())), preferred_element_type=F32)


def fold_rows(v):
    return jnp.sum(v.reshape(v.shape[0] // 8, 8, v.shape[1]), axis=0)


def elu(v):
    return jnp.where(v > 0, v, jnp.exp(jnp.minimum(v, 0.0)) - 1.0)


def fused(
    n,
    pair_hbm, feats_hbm, w_row_hbm, w_col_hbm, taps1_hbm, taps2_hbm, scale_hbm, shift_hbm,
    out,
    feats, w_row, w_col, taps1, taps2, scale, shift,
    pair_up, pair_dn, halo_up, halo_dn, p32, h32, all_feats, own_w, halo_w, col_conv, col_base, acc,
    edges, stats, block, mirror, m32, o32, out_v,
    in_sem, feat_s, feat_r, stat_s, stat_r, edge_s, edge_r, mir_s, mir_r, out_sem,
):
    me = lax.axis_index("gx")
    ch, _, cols = pair_up.shape
    rows = 2 * D
    half = n // 2
    side = lax.div(me, half)
    lane = lax.rem(me, half)
    cells = float(n * rows * cols)
    low = low_half()

    def peer_of(k):
        return lax.rem(side + 1 + lax.div(k, half), 2) * half + lax.rem(lane + k, half)

    def sender_of(k):
        return lax.rem(side + 1 + lax.div(k, half), 2) * half + lax.rem(lane + n - k, half)

    def far_peers(act):
        pl.loop(0, half)(act)

    def near_peers(act):
        pl.loop(half + 1, n)(act)

    def all_peers(act):
        far_peers(act)
        near_peers(act)

    barrier = pltpu.get_barrier_semaphore()

    @all_peers
    def _(k):
        pl.semaphore_signal(barrier, inc=1, device_id={"gx": peer_of(k)}, device_id_type=MESH)

    loads = [
        pltpu.make_async_copy(src, dst, in_sem.at[k])
        for k, (src, dst) in enumerate(
            (
                (feats_hbm, feats), (pair_hbm.at[:, pl.ds(0, D), :], pair_up),
                (pair_hbm.at[:, pl.ds(D, D), :], pair_dn), (w_row_hbm, w_row), (w_col_hbm, w_col),
                (taps1_hbm, taps1), (taps2_hbm, taps2), (scale_hbm, scale), (shift_hbm, shift),
            )
        )
    ]
    for load in loads:
        load.start()
    for load in loads[:3]:
        load.wait()
    pl.semaphore_wait(barrier, n - 1)

    def copy_to(src, dst, s, r, peer):
        return pltpu.make_async_remote_copy(
            src_ref=src, dst_ref=dst, send_sem=s, recv_sem=r,
            device_id={"gx": peer}, device_id_type=MESH,
        )

    def feat_copy(k):
        return copy_to(feats, all_feats.at[me], feat_s.at[k], feat_r.at[k], peer_of(k))

    def stat_copy(index, k):
        return copy_to(
            stats.at[index, me], stats.at[index, me], stat_s.at[index, k], stat_r.at[index, k],
            peer_of(k),
        )

    def mirror_copy(k):
        peer = peer_of(k)
        start = pl.multiple_of(peer * rows, rows)
        return copy_to(
            block.at[:, pl.ds(start, rows), :], mirror.at[me], mir_s.at[k], mir_r.at[k], peer
        )

    def edge_copies(index):
        above, below = jnp.maximum(me - 1, 0), jnp.minimum(me + 1, n - 1)
        s, r = edge_s.at[index], edge_r.at[index]
        if index == 0:
            return (
                copy_to(pair_up, halo_dn, s.at[0], r.at[0], above),
                copy_to(pair_dn, halo_up, s.at[1], r.at[1], below),
            )
        return (
            copy_to(edges.at[0], edges.at[3], s.at[0], r.at[0], above),
            copy_to(edges.at[1], edges.at[2], s.at[1], r.at[1], below),
        )

    def edges_start(index):
        first, second = edge_copies(index)

        @pl.when(me > 0)
        def _():
            first.start()

        @pl.when(me < n - 1)
        def _():
            second.start()

    def edges_wait_recv(index):
        first, second = edge_copies(index)

        @pl.when(me < n - 1)
        def _():
            first.wait_recv()

        @pl.when(me > 0)
        def _():
            second.wait_recv()

    def edges_wait_send(index):
        first, second = edge_copies(index)

        @pl.when(me > 0)
        def _():
            first.wait_send()

        @pl.when(me < n - 1)
        def _():
            second.wait_send()

    @all_peers
    def _(k):
        feat_copy(k).start()

    edges_start(0)
    all_feats[me] = feats[...]

    for load in loads[3:]:
        load.wait()

    def rounded(a, w):
        return times(a, w).astype(BF).astype(F32)

    w_row2 = jnp.concatenate([w_row[...]] * 2, axis=0)
    w_col2 = jnp.concatenate([w_col[...]] * 2, axis=0)
    own_rows = rounded(feats[...], w_row2)
    own_rows = jnp.where(low, own_rows[:D], own_rows[D:])
    halves = cols // 128
    for h in range(halves):
        where = slice(h * 128, h * 128 + 128)
        p32[h, 0] = pair_up[:, :, where].astype(F32).reshape(ch * D, 128)
        p32[h, 1] = pair_dn[:, :, where].astype(F32).reshape(ch * D, 128)

    def pick(values, i):
        chosen = lax.broadcasted_iota(jnp.int32, values.shape, 0) == i
        return jnp.sum(jnp.where(chosen, values, 0.0), axis=0, keepdims=True)

    def with_rows(source, row_values, i):
        parts = []
        for h in range(halves):
            first = source[h, 0, pl.ds(i, ch, stride=D), :]
            second = source[h, 1, pl.ds(i, ch, stride=D), :]
            parts.append(jnp.concatenate([first, second], axis=0).T)
        return jnp.concatenate(parts, axis=0) + pick(row_values, i)

    def pack(i, early, late):
        edges[0, i] = jnp.where(low, early, half_roll(late)).astype(BF)
        edges[1, i] = jnp.where(low, half_roll(early), late).astype(BF)

    for index, taps in enumerate((taps1, taps2)):
        t = taps[...].astype(F32)
        none = jnp.zeros_like(t[0])
        for kx in range(3):
            where = slice(kx * 128, kx * 128 + 128)
            top = jnp.concatenate([t[3 + kx], t[6 + kx]], axis=1)
            bottom = jnp.concatenate([t[kx], t[3 + kx]], axis=1)
            own_w[index, :, where] = jnp.concatenate([top, bottom], axis=0).astype(BF)
            top = jnp.concatenate([t[kx], none], axis=1)
            bottom = jnp.concatenate([none, t[6 + kx]], axis=1)
            halo_w[index, :, where] = jnp.concatenate([top, bottom], axis=0).astype(BF)

    @pl.loop(0, D)
    def _(i):
        v = with_rows(p32, own_rows, i)
        block[i] = v.astype(BF)
        acc[i] = times(three_shifts(v), own_w[0])

    @all_peers
    def _(k):
        feat_copy(k).wait_recv()

    inside = jnp.where(low, (me > 0).astype(F32), (me < n - 1).astype(F32)) > 0.5
    col_part = rounded(all_feats[...].reshape(n * rows, feats.shape[1]), w_col2)
    col_conv[...] = times(three_shifts(col_part), own_w[0]) + times(
        three_shifts(jnp.where(inside, col_part, 0.0)), halo_w[0]
    )
    col_base[...] = col_part + jnp.concatenate([shift[1:2, :]] * 2, axis=1)

    def unpacked(i):
        u = edges[2, i].astype(F32)
        d = edges[3, i].astype(F32)
        return jnp.where(low, u, half_roll(d)), jnp.where(low, half_roll(u), d)

    def add_sums(sums, a):
        return sums[0] + fold_rows(a), sums[1] + fold_rows(a * a)

    zeros = jnp.zeros((8, 128), F32)

    def publish(index, sums):
        lines = []
        for v in sums:
            v = jnp.sum(v, axis=0, keepdims=True)
            lines.append(v + half_roll(v))
        stats[index, me] = jnp.concatenate(lines + [jnp.zeros((6, 128), F32)], axis=0)

        @all_peers
        def _(k):
            stat_copy(index, k).start()

    def collect(index):
        @all_peers
        def _(k):
            stat_copy(index, k).wait_recv()

        total = jnp.sum(stats[index], axis=0)
        average = total[0:1] / cells
        spread = total[1:2] / cells - average * average
        gain = jnp.concatenate([scale[index : index + 1, :]] * 2, axis=1)
        return average, gain * lax.rsqrt(spread + epsilon)

    rows_up = rounded(all_feats[jnp.maximum(me - 1, 0)], w_row2)[D:]
    rows_dn = rounded(all_feats[jnp.minimum(me + 1, n - 1)], w_row2)[:D]
    halo_rows = jnp.where(low, rows_up, rows_dn)

    edges_wait_recv(0)
    for h in range(halves):
        where = slice(h * 128, h * 128 + 128)
        h32[h, 0] = halo_up[:, :, where].astype(F32).reshape(ch * D, 128)
        h32[h, 1] = halo_dn[:, :, where].astype(F32).reshape(ch * D, 128)

    def first_edge(i, sums):
        results = []
        for offset in (0, D // 2):
            v = jnp.where(inside, with_rows(h32, halo_rows, i + offset), 0.0)
            a = acc[i + offset] + times(three_shifts(v), halo_w[0]) + col_conv[...]
            acc[i + offset] = a
            sums = add_sums(sums, a)
            results.append(a)
        pack(i, *results)
        return sums

    sums = lax.fori_loop(0, D // 2, first_edge, (zeros, zeros))
    publish(0, sums)
    edges_start(1)
    average, factor = collect(0)
    base = jnp.concatenate([shift[0:1, :]] * 2, axis=1)

    @pl.loop(0, D)
    def _(i):
        a = elu((acc[i] - average) * factor + base)
        acc[i] = times(three_shifts(a), own_w[1])

    edges_wait_recv(1)

    def second_edge(i, sums):
        for offset, v in zip((0, D // 2), unpacked(i)):
            v = jnp.where(inside, elu((v - average) * factor + base), 0.0)
            a = acc[i + offset] + times(three_shifts(v), halo_w[1])
            acc[i + offset] = a
            sums = add_sums(sums, a)
        return sums

    sums = lax.fori_loop(0, D // 2, second_edge, (zeros, zeros))
    publish(1, sums)
    average2, factor2 = collect(1)

    def result_of(which):
        where = pl.ds(pl.multiple_of(which * 128, 128), 128)

        @pl.loop(0, D)
        def _(i):
            v = block[i, where, :].astype(F32) + col_base[where, :]
            v = v + (acc[i, where, :] - average2) * factor2
            block[i, where, :] = elu(v).astype(BF)

    def widen(e):
        start = pl.multiple_of(e * (D * rows), D * rows)
        m32[pl.ds(start, D * rows), :] = mirror[e].astype(F32).reshape(D * rows, 128)

    def finish(which):
        where = pl.ds(pl.multiple_of(which * 128, 128), 128)
        offset = which * (half * D * rows)

        @pl.loop(0, D)
        def _(i):
            first = m32[pl.ds(offset + i, half * D, stride=rows), :]
            second = m32[pl.ds(offset + i + D, half * D, stride=rows), :]
            even = jnp.where(low, first, half_roll(second)).reshape(half, 1, D, 128)
            odd = jnp.where(low, half_roll(first), second).reshape(half, 1, D, 128)
            m = jnp.concatenate([even, odd], axis=1).reshape(128, 128)
            t = (0.5 * (block[i, where, :].astype(F32) + m)).T
            o32[which, pl.ds(i, ch, stride=rows), :] = t[:ch]
            o32[which, pl.ds(i + D, ch, stride=rows), :] = t[ch:]

        out_v[which] = o32[which].reshape(ch, rows, 128).astype(BF)
        copy = pltpu.make_async_copy(out_v.at[which], out.at[:, :, where], out_sem.at[which])
        copy.start()
        return copy

    result_of(1 - side)

    @far_peers
    def _(k):
        mirror_copy(k).start()

    result_of(side)

    @near_peers
    def _(k):
        mirror_copy(k).start()

    mirror[me] = block[:, pl.ds(pl.multiple_of(me * rows, rows), rows), :]
    widen(me)

    @near_peers
    def _(k):
        mirror_copy(k).wait_recv()
        widen(sender_of(k))

    near = finish(side)

    @all_peers
    def _(k):
        feat_copy(k).wait_send()
        stat_copy(0, k).wait_send()
        stat_copy(1, k).wait_send()

    edges_wait_send(0)
    edges_wait_send(1)

    @far_peers
    def _(k):
        mirror_copy(k).wait_recv()
        widen(sender_of(k))

    far = finish(1 - side)

    @all_peers
    def _(k):
        mirror_copy(k).wait_send()

    near.wait()
    far.wait()


def fused_body(n, *args):
    residue_feats, pair_feats = args[:2]
    ch, rows, cols = pair_feats.shape
    halves = cols // 128
    rest = (args[2].T, args[3].T) + args[4:]
    dma = pltpu.SemaphoreType.DMA
    return pl.pallas_call(
        functools.partial(fused, n),
        out_shape=jax.ShapeDtypeStruct(pair_feats.shape, BF),
        in_specs=[pl.BlockSpec(memory_space=pltpu.HBM)] * 8,
        out_specs=pl.BlockSpec(memory_space=pl.ANY),
        scratch_shapes=[
            *[pltpu.VMEM(a.shape, a.dtype) for a in (residue_feats,) + rest],
            *[pltpu.VMEM((ch, D, cols), BF)] * 4,
            *[pltpu.VMEM((halves, 2, ch * D, 128), F32)] * 2,
            pltpu.VMEM((n,) + residue_feats.shape, BF),
            pltpu.VMEM((2, 128, 384), BF),
            pltpu.VMEM((2, 128, 384), BF),
            pltpu.VMEM((cols, 128), F32),
            pltpu.VMEM((cols, 128), F32),
            pltpu.VMEM((D, cols, 128), F32),
            pltpu.VMEM((4, D // 2, cols, 128), BF),
            pltpu.VMEM((2, n, 8, 128), F32),
            pltpu.VMEM((D, cols, 128), BF),
            pltpu.VMEM((n, D, rows, 128), BF),
            pltpu.VMEM((n * D * rows, 128), F32),
            pltpu.VMEM((halves, ch * rows, 128), F32),
            pltpu.VMEM((halves, ch, rows, 128), BF),
            dma((9,)),
            dma((n,)), dma((n,)), dma((2, n)), dma((2, n)), dma((2, 2)), dma((2, 2)),
            dma((n,)), dma((n,)), dma((2,)),
        ],
        compiler_params=pltpu.CompilerParams(
            collective_id=0, has_side_effects=True, vmem_limit_bytes=63 * 1024 * 1024
        ),
    )(pair_feats, residue_feats, *rest)


def solution(mesh):
    placed = (P(("grp", "gx"), None), P(None, ("grp", "gx"), "gy"), P(), P(), P(), P(), P(), P())
    n = mesh.shape["gx"]

    def chosen(*args):
        ch, rows, cols = args[1].shape
        fits = mesh.shape["gy"] == 1 and rows == 2 * D and cols == n * rows
        if fits and ch == 64 and cols == 256:
            return fused_body(n, *args)
        return body(*args)

    return jax.shard_map(
        chosen, mesh=mesh, in_specs=placed, out_specs=P(None, ("grp", "gx"), "gy"), check_vma=False
    )
```

```python
import functools

import jax
import jax.numpy as jnp
from jax import lax
from jax.experimental import pallas as pl
from jax.experimental.pallas import tpu as pltpu
from jax.sharding import PartitionSpec as P

DILATION_STEP = 8


epsilon = 1e-05


def with_halo(cells, sides, width):
    for axis, dim in sides:
        count = lax.axis_size(axis)
        ends = count - 1
        head = lax.slice_in_dim(cells, 0, width, axis=dim)
        tail = lax.slice_in_dim(cells, cells.shape[dim] - width, cells.shape[dim], axis=dim)
        cells = jnp.concatenate(
            [
                lax.ppermute(tail, axis, [(i, (i + 1) % count) for i in range(ends)]),
                cells,
                lax.ppermute(head, axis, [((i + 1) % count, i) for i in range(ends)]),
            ],
            axis=dim,
        )
    return cells


def dilated(receptive_region, weights):
    row_count = receptive_region.shape[1]
    col_count = receptive_region.shape[2]
    border_padded_input = with_halo(receptive_region, (("gx", 1), ("gy", 2)), DILATION_STEP)
    tap_sum_total = jnp.zeros((weights.shape[1], row_count, col_count), jnp.float32)
    for filter_tap_index in range(9):
        row_displacement = filter_tap_index // 3 * DILATION_STEP
        column_displacement = filter_tap_index % 3 * DILATION_STEP
        window = border_padded_input[
            :,
            row_displacement : row_displacement + row_count,
            column_displacement : column_displacement + col_count,
        ]
        tap_sum_total = tap_sum_total + jnp.einsum(
            "oc,crw->orw", weights[filter_tap_index], window, preferred_element_type=jnp.float32
        )
    return tap_sum_total


def normalized(tap_sum_total, gain, shift):
    cell_count = (
        tap_sum_total.shape[1] * tap_sum_total.shape[2] * lax.axis_size("gx") * lax.axis_size("gy")
    )
    first_sum, second_sum = lax.psum(
        (jnp.sum(tap_sum_total, axis=(1, 2)), jnp.sum(tap_sum_total * tap_sum_total, axis=(1, 2))),
        ("gx", "gy"),
    )
    average = first_sum / cell_count
    spread = second_sum / cell_count - average * average
    centred = tap_sum_total - average[:, None, None]
    factor = gain * lax.rsqrt(spread + epsilon)
    return centred * factor[:, None, None] + shift[:, None, None]


def body(residue_feats, pair_feats, w_row, w_col, first_taps, second_taps, norm_scale, norm_shift):
    col_count = pair_feats.shape[2]
    col_start = lax.axis_index("gy") * col_count
    row_part = jnp.dot(residue_feats, w_row, preferred_element_type=jnp.float32).astype(
        jnp.bfloat16
    )
    everyone = lax.all_gather(residue_feats, "gx", axis=0, tiled=True)
    col_feats = lax.dynamic_slice_in_dim(everyone, col_start, col_count, 0)
    col_part = jnp.dot(col_feats, w_col, preferred_element_type=jnp.float32).astype(jnp.bfloat16)
    block_in = (
        pair_feats.astype(jnp.float32)
        + row_part.T.astype(jnp.float32)[:, :, None]
        + col_part.T.astype(jnp.float32)[:, None, :]
    ).astype(jnp.bfloat16)
    first_conv = dilated(block_in, first_taps)
    activated = jax.nn.elu(normalized(first_conv, norm_scale[0], norm_shift[0])).astype(
        jnp.bfloat16
    )
    second_conv = dilated(activated, second_taps)
    block_out = jax.nn.elu(
        block_in.astype(jnp.float32) + normalized(second_conv, norm_scale[1], norm_shift[1])
    ).astype(jnp.bfloat16)
    whole_rows = lax.all_gather(block_out, "gy", axis=2, tiled=True)
    columns = lax.all_to_all(whole_rows, "gx", split_axis=2, concat_axis=1, tiled=True)
    flipped = lax.dynamic_slice_in_dim(columns, col_start, col_count, 1)
    mirrored = jnp.transpose(flipped, (0, 2, 1))
    return (0.5 * (block_out.astype(jnp.float32) + mirrored.astype(jnp.float32))).astype(
        jnp.bfloat16
    )


MESH = pl.DeviceIdType.MESH
D = DILATION_STEP
BF = jnp.bfloat16
F32 = jnp.float32


def low_half():
    return lax.broadcasted_iota(jnp.int32, (1, 128), 1) < 64


def half_roll(v):
    return pltpu.roll(v, 64, 1)


def three_shifts(v):
    gap = jnp.zeros((D, v.shape[1]), v.dtype)
    left = jnp.concatenate([gap, v[:-D]], axis=0)
    right = jnp.concatenate([v[D:], gap], axis=0)
    return jnp.concatenate([left.astype(BF), v.astype(BF), right.astype(BF)], axis=1)


def times(a, w):
    return lax.dot_general(a, w, (((1,), (1,)), ((), ())), preferred_element_type=F32)


def fold_rows(v):
    return jnp.sum(v.reshape(v.shape[0] // 8, 8, v.shape[1]), axis=0)


def elu(v):
    return jnp.where(v > 0, v, jnp.exp(jnp.minimum(v, 0.0)) - 1.0)


def fused(
    n,
    pair_hbm, feats_hbm, w_row_hbm, w_col_hbm, taps1_hbm, taps2_hbm, scale_hbm, shift_hbm,
    out,
    feats, w_row, w_col, taps1, taps2, scale, shift,
    pair_up, pair_dn, halo_up, halo_dn, p32, h32, all_feats, own_w, halo_w, col_conv, col_base, acc,
    edges, stats, block, tiles, mirror, m32, o32, out_v,
    in_sem, feat_s, feat_r, stat_s, stat_r, edge_s, edge_r, mir_s, mir_r, out_sem,
):
    me = lax.axis_index("gx")
    ch, _, cols = pair_up.shape
    rows = 2 * D
    half = n // 2
    side = lax.div(me, half)
    lane = lax.rem(me, half)
    cells = float(n * rows * cols)
    low = low_half()

    def peer_of(k):
        return lax.rem(side + 1 + lax.div(k, half), 2) * half + lax.rem(lane + k, half)

    def sender_of(k):
        return lax.rem(side + 1 + lax.div(k, half), 2) * half + lax.rem(lane + n - k, half)

    def far_peers(act):
        pl.loop(0, half)(act)

    def near_peers(act):
        pl.loop(half + 1, n)(act)

    def all_peers(act):
        far_peers(act)
        near_peers(act)

    barrier = pltpu.get_barrier_semaphore()

    @all_peers
    def _(k):
        pl.semaphore_signal(barrier, inc=1, device_id={"gx": peer_of(k)}, device_id_type=MESH)

    loads = [
        pltpu.make_async_copy(src, dst, in_sem.at[k])
        for k, (src, dst) in enumerate(
            (
                (feats_hbm, feats), (pair_hbm.at[:, pl.ds(0, D), :], pair_up),
                (pair_hbm.at[:, pl.ds(D, D), :], pair_dn), (w_row_hbm, w_row), (w_col_hbm, w_col),
                (taps1_hbm, taps1), (taps2_hbm, taps2), (scale_hbm, scale), (shift_hbm, shift),
            )
        )
    ]
    for load in loads:
        load.start()
    for load in loads[:3]:
        load.wait()
    pl.semaphore_wait(barrier, n - 1)

    def copy_to(src, dst, s, r, peer):
        return pltpu.make_async_remote_copy(
            src_ref=src, dst_ref=dst, send_sem=s, recv_sem=r,
            device_id={"gx": peer}, device_id_type=MESH,
        )

    def feat_copy(k):
        return copy_to(feats, all_feats.at[me], feat_s.at[k], feat_r.at[k], peer_of(k))

    def stat_copy(index, k):
        return copy_to(
            stats.at[index, me], stats.at[index, me], stat_s.at[index, k], stat_r.at[index, k],
            peer_of(k),
        )

    def mirror_copy(k):
        peer = peer_of(k)
        return copy_to(tiles.at[peer], mirror.at[me], mir_s.at[k], mir_r.at[k], peer)

    def edge_copies(index):
        above, below = jnp.maximum(me - 1, 0), jnp.minimum(me + 1, n - 1)
        s, r = edge_s.at[index], edge_r.at[index]
        if index == 0:
            return (
                copy_to(pair_up, halo_dn, s.at[0], r.at[0], above),
                copy_to(pair_dn, halo_up, s.at[1], r.at[1], below),
            )
        return (
            copy_to(edges.at[0], edges.at[3], s.at[0], r.at[0], above),
            copy_to(edges.at[1], edges.at[2], s.at[1], r.at[1], below),
        )

    def edges_start(index):
        first, second = edge_copies(index)

        @pl.when(me > 0)
        def _():
            first.start()

        @pl.when(me < n - 1)
        def _():
            second.start()

    def edges_wait_recv(index):
        first, second = edge_copies(index)

        @pl.when(me < n - 1)
        def _():
            first.wait_recv()

        @pl.when(me > 0)
        def _():
            second.wait_recv()

    def edges_wait_send(index):
        first, second = edge_copies(index)

        @pl.when(me > 0)
        def _():
            first.wait_send()

        @pl.when(me < n - 1)
        def _():
            second.wait_send()

    @all_peers
    def _(k):
        feat_copy(k).start()

    edges_start(0)
    all_feats[me] = feats[...]

    for load in loads[3:]:
        load.wait()

    def rounded(a, w):
        return times(a, w).astype(BF).astype(F32)

    w_row2 = jnp.concatenate([w_row[...]] * 2, axis=0)
    w_col2 = jnp.concatenate([w_col[...]] * 2, axis=0)
    own_rows = rounded(feats[...], w_row2)
    own_rows = jnp.where(low, own_rows[:D], own_rows[D:])
    halves = cols // 128
    for h in range(halves):
        where = slice(h * 128, h * 128 + 128)
        p32[h, 0] = pair_up[:, :, where].astype(F32).reshape(ch * D, 128)
        p32[h, 1] = pair_dn[:, :, where].astype(F32).reshape(ch * D, 128)

    def pick(values, i):
        chosen = lax.broadcasted_iota(jnp.int32, values.shape, 0) == i
        return jnp.sum(jnp.where(chosen, values, 0.0), axis=0, keepdims=True)

    def with_rows(source, row_values, i):
        parts = []
        for h in range(halves):
            first = source[h, 0, pl.ds(i, ch, stride=D), :]
            second = source[h, 1, pl.ds(i, ch, stride=D), :]
            parts.append(jnp.concatenate([first, second], axis=0).T)
        return jnp.concatenate(parts, axis=0) + pick(row_values, i)

    def pack(i, early, late):
        edges[0, i] = jnp.where(low, early, half_roll(late)).astype(BF)
        edges[1, i] = jnp.where(low, half_roll(early), late).astype(BF)

    for index, taps in enumerate((taps1, taps2)):
        t = taps[...].astype(F32)
        none = jnp.zeros_like(t[0])
        for kx in range(3):
            where = slice(kx * 128, kx * 128 + 128)
            top = jnp.concatenate([t[3 + kx], t[6 + kx]], axis=1)
            bottom = jnp.concatenate([t[kx], t[3 + kx]], axis=1)
            own_w[index, :, where] = jnp.concatenate([top, bottom], axis=0).astype(BF)
            top = jnp.concatenate([t[kx], none], axis=1)
            bottom = jnp.concatenate([none, t[6 + kx]], axis=1)
            halo_w[index, :, where] = jnp.concatenate([top, bottom], axis=0).astype(BF)

    @pl.loop(0, D, unroll=D)
    def _(i):
        v = with_rows(p32, own_rows, i)
        block[i] = v.astype(BF)
        acc[i] = times(three_shifts(v), own_w[0])

    @all_peers
    def _(k):
        feat_copy(k).wait_recv()

    inside = jnp.where(low, (me > 0).astype(F32), (me < n - 1).astype(F32)) > 0.5
    col_part = rounded(all_feats[...].reshape(n * rows, feats.shape[1]), w_col2)
    col_conv[...] = times(three_shifts(col_part), own_w[0]) + times(
        three_shifts(jnp.where(inside, col_part, 0.0)), halo_w[0]
    )
    col_base[...] = col_part + jnp.concatenate([shift[1:2, :]] * 2, axis=1)

    def unpacked(i):
        u = edges[2, i].astype(F32)
        d = edges[3, i].astype(F32)
        return jnp.where(low, u, half_roll(d)), jnp.where(low, half_roll(u), d)

    def add_sums(sums, a):
        return sums[0] + fold_rows(a), sums[1] + fold_rows(a * a)

    zeros = jnp.zeros((8, 128), F32)

    def publish(index, sums):
        lines = []
        for v in sums:
            v = jnp.sum(v, axis=0, keepdims=True)
            lines.append(v + half_roll(v))
        stats[index, me] = jnp.concatenate(lines + [jnp.zeros((6, 128), F32)], axis=0)

        @all_peers
        def _(k):
            stat_copy(index, k).start()

    def collect(index):
        @all_peers
        def _(k):
            stat_copy(index, k).wait_recv()

        total = jnp.sum(stats[index], axis=0)
        average = total[0:1] / cells
        spread = total[1:2] / cells - average * average
        gain = jnp.concatenate([scale[index : index + 1, :]] * 2, axis=1)
        return average, gain * lax.rsqrt(spread + epsilon)

    rows_up = rounded(all_feats[jnp.maximum(me - 1, 0)], w_row2)[D:]
    rows_dn = rounded(all_feats[jnp.minimum(me + 1, n - 1)], w_row2)[:D]
    halo_rows = jnp.where(low, rows_up, rows_dn)

    edges_wait_recv(0)
    for h in range(halves):
        where = slice(h * 128, h * 128 + 128)
        h32[h, 0] = halo_up[:, :, where].astype(F32).reshape(ch * D, 128)
        h32[h, 1] = halo_dn[:, :, where].astype(F32).reshape(ch * D, 128)

    def first_edge(i, sums):
        results = []
        for offset in (0, D // 2):
            v = jnp.where(inside, with_rows(h32, halo_rows, i + offset), 0.0)
            a = acc[i + offset] + times(three_shifts(v), halo_w[0]) + col_conv[...]
            acc[i + offset] = a
            sums = add_sums(sums, a)
            results.append(a)
        pack(i, *results)
        return sums

    sums = lax.fori_loop(0, D // 2, first_edge, (zeros, zeros), unroll=D // 2)
    publish(0, sums)
    edges_start(1)
    average, factor = collect(0)
    base = jnp.concatenate([shift[0:1, :]] * 2, axis=1)

    @pl.loop(0, D, unroll=D)
    def _(i):
        a = elu((acc[i] - average) * factor + base)
        acc[i] = times(three_shifts(a), own_w[1])

    edges_wait_recv(1)

    def second_edge(i, sums):
        for offset, v in zip((0, D // 2), unpacked(i)):
            v = jnp.where(inside, elu((v - average) * factor + base), 0.0)
            a = acc[i + offset] + times(three_shifts(v), halo_w[1])
            acc[i + offset] = a
            sums = add_sums(sums, a)
        return sums

    sums = lax.fori_loop(0, D // 2, second_edge, (zeros, zeros), unroll=D // 2)
    publish(1, sums)
    average2, factor2 = collect(1)

    def result_of(which):
        where = pl.ds(pl.multiple_of(which * 128, 128), 128)

        @pl.loop(0, D, unroll=D)
        def _(i):
            v = block[i, where, :].astype(F32) + col_base[where, :]
            v = v + (acc[i, where, :] - average2) * factor2
            tiles[pl.ds(which * half, half), i] = elu(v).astype(BF).reshape(half, rows, 128)

    def widen(e):
        start = pl.multiple_of(e * (D * rows), D * rows)
        m32[pl.ds(start, D * rows), :] = mirror[e].astype(F32).reshape(D * rows, 128)

    def finish(which):
        where = pl.ds(pl.multiple_of(which * 128, 128), 128)
        offset = which * (half * D * rows)

        @pl.loop(0, D, unroll=D)
        def _(i):
            first = m32[pl.ds(offset + i, half * D, stride=rows), :]
            second = m32[pl.ds(offset + i + D, half * D, stride=rows), :]
            even = jnp.where(low, first, half_roll(second)).reshape(half, 1, D, 128)
            odd = jnp.where(low, half_roll(first), second).reshape(half, 1, D, 128)
            m = jnp.concatenate([even, odd], axis=1).reshape(128, 128)
            own = tiles[pl.ds(which * half, half), i].astype(F32).reshape(128, 128)
            t = (0.5 * (own + m)).T
            o32[which, pl.ds(i, ch, stride=rows), :] = t[:ch]
            o32[which, pl.ds(i + D, ch, stride=rows), :] = t[ch:]

        out_v[which] = o32[which].reshape(ch, rows, 128).astype(BF)
        copy = pltpu.make_async_copy(out_v.at[which], out.at[:, :, where], out_sem.at[which])
        copy.start()
        return copy

    result_of(1 - side)

    @far_peers
    def _(k):
        mirror_copy(k).start()

    result_of(side)

    @near_peers
    def _(k):
        mirror_copy(k).start()

    mirror[me] = tiles[me]
    widen(me)

    @near_peers
    def _(k):
        mirror_copy(k).wait_recv()
        widen(sender_of(k))

    near = finish(side)

    @all_peers
    def _(k):
        feat_copy(k).wait_send()
        stat_copy(0, k).wait_send()
        stat_copy(1, k).wait_send()

    edges_wait_send(0)
    edges_wait_send(1)

    @far_peers
    def _(k):
        mirror_copy(k).wait_recv()
        widen(sender_of(k))

    far = finish(1 - side)

    @all_peers
    def _(k):
        mirror_copy(k).wait_send()

    near.wait()
    far.wait()


def fused_body(n, *args):
    residue_feats, pair_feats = args[:2]
    ch, rows, cols = pair_feats.shape
    halves = cols // 128
    rest = (args[2].T, args[3].T) + args[4:]
    dma = pltpu.SemaphoreType.DMA
    return pl.pallas_call(
        functools.partial(fused, n),
        out_shape=jax.ShapeDtypeStruct(pair_feats.shape, BF),
        in_specs=[pl.BlockSpec(memory_space=pltpu.HBM)] * 8,
        out_specs=pl.BlockSpec(memory_space=pl.ANY),
        scratch_shapes=[
            *[pltpu.VMEM(a.shape, a.dtype) for a in (residue_feats,) + rest],
            *[pltpu.VMEM((ch, D, cols), BF)] * 4,
            *[pltpu.VMEM((halves, 2, ch * D, 128), F32)] * 2,
            pltpu.VMEM((n,) + residue_feats.shape, BF),
            pltpu.VMEM((2, 128, 384), BF),
            pltpu.VMEM((2, 128, 384), BF),
            pltpu.VMEM((cols, 128), F32),
            pltpu.VMEM((cols, 128), F32),
            pltpu.VMEM((D, cols, 128), F32),
            pltpu.VMEM((4, D // 2, cols, 128), BF),
            pltpu.VMEM((2, n, 8, 128), F32),
            pltpu.VMEM((D, cols, 128), BF),
            *[pltpu.VMEM((n, D, rows, 128), BF)] * 2,
            pltpu.VMEM((n * D * rows, 128), F32),
            pltpu.VMEM((halves, ch * rows, 128), F32),
            pltpu.VMEM((halves, ch, rows, 128), BF),
            dma((9,)),
            dma((n,)), dma((n,)), dma((2, n)), dma((2, n)), dma((2, 2)), dma((2, 2)),
            dma((n,)), dma((n,)), dma((2,)),
        ],
        compiler_params=pltpu.CompilerParams(
            collective_id=0, has_side_effects=True, vmem_limit_bytes=63 * 1024 * 1024
        ),
    )(pair_feats, residue_feats, *rest)


def solution(mesh):
    placed = (P(("grp", "gx"), None), P(None, ("grp", "gx"), "gy"), P(), P(), P(), P(), P(), P())
    n = mesh.shape["gx"]

    def chosen(*args):
        ch, rows, cols = args[1].shape
        fits = mesh.shape["gy"] == 1 and rows == 2 * D and cols == n * rows
        if fits and ch == 64 and cols == 256:
            return fused_body(n, *args)
        return body(*args)

    return jax.shard_map(
        chosen, mesh=mesh, in_specs=placed, out_specs=P(None, ("grp", "gx"), "gy"), check_vma=False
    )
```

```python
import functools

import jax
import jax.numpy as jnp
from jax import lax
from jax.experimental import pallas as pl
from jax.experimental.pallas import tpu as pltpu
from jax.sharding import PartitionSpec as P

DILATION_STEP = 8


epsilon = 1e-05


def with_halo(cells, sides, width):
    for axis, dim in sides:
        count = lax.axis_size(axis)
        ends = count - 1
        head = lax.slice_in_dim(cells, 0, width, axis=dim)
        tail = lax.slice_in_dim(cells, cells.shape[dim] - width, cells.shape[dim], axis=dim)
        cells = jnp.concatenate(
            [
                lax.ppermute(tail, axis, [(i, (i + 1) % count) for i in range(ends)]),
                cells,
                lax.ppermute(head, axis, [((i + 1) % count, i) for i in range(ends)]),
            ],
            axis=dim,
        )
    return cells


def dilated(receptive_region, weights):
    row_count = receptive_region.shape[1]
    col_count = receptive_region.shape[2]
    border_padded_input = with_halo(receptive_region, (("gx", 1), ("gy", 2)), DILATION_STEP)
    tap_sum_total = jnp.zeros((weights.shape[1], row_count, col_count), jnp.float32)
    for filter_tap_index in range(9):
        row_displacement = filter_tap_index // 3 * DILATION_STEP
        column_displacement = filter_tap_index % 3 * DILATION_STEP
        window = border_padded_input[
            :,
            row_displacement : row_displacement + row_count,
            column_displacement : column_displacement + col_count,
        ]
        tap_sum_total = tap_sum_total + jnp.einsum(
            "oc,crw->orw", weights[filter_tap_index], window, preferred_element_type=jnp.float32
        )
    return tap_sum_total


def normalized(tap_sum_total, gain, shift):
    cell_count = (
        tap_sum_total.shape[1] * tap_sum_total.shape[2] * lax.axis_size("gx") * lax.axis_size("gy")
    )
    first_sum, second_sum = lax.psum(
        (jnp.sum(tap_sum_total, axis=(1, 2)), jnp.sum(tap_sum_total * tap_sum_total, axis=(1, 2))),
        ("gx", "gy"),
    )
    average = first_sum / cell_count
    spread = second_sum / cell_count - average * average
    centred = tap_sum_total - average[:, None, None]
    factor = gain * lax.rsqrt(spread + epsilon)
    return centred * factor[:, None, None] + shift[:, None, None]


def body(residue_feats, pair_feats, w_row, w_col, first_taps, second_taps, norm_scale, norm_shift):
    col_count = pair_feats.shape[2]
    col_start = lax.axis_index("gy") * col_count
    row_part = jnp.dot(residue_feats, w_row, preferred_element_type=jnp.float32).astype(
        jnp.bfloat16
    )
    everyone = lax.all_gather(residue_feats, "gx", axis=0, tiled=True)
    col_feats = lax.dynamic_slice_in_dim(everyone, col_start, col_count, 0)
    col_part = jnp.dot(col_feats, w_col, preferred_element_type=jnp.float32).astype(jnp.bfloat16)
    block_in = (
        pair_feats.astype(jnp.float32)
        + row_part.T.astype(jnp.float32)[:, :, None]
        + col_part.T.astype(jnp.float32)[:, None, :]
    ).astype(jnp.bfloat16)
    first_conv = dilated(block_in, first_taps)
    activated = jax.nn.elu(normalized(first_conv, norm_scale[0], norm_shift[0])).astype(
        jnp.bfloat16
    )
    second_conv = dilated(activated, second_taps)
    block_out = jax.nn.elu(
        block_in.astype(jnp.float32) + normalized(second_conv, norm_scale[1], norm_shift[1])
    ).astype(jnp.bfloat16)
    whole_rows = lax.all_gather(block_out, "gy", axis=2, tiled=True)
    columns = lax.all_to_all(whole_rows, "gx", split_axis=2, concat_axis=1, tiled=True)
    flipped = lax.dynamic_slice_in_dim(columns, col_start, col_count, 1)
    mirrored = jnp.transpose(flipped, (0, 2, 1))
    return (0.5 * (block_out.astype(jnp.float32) + mirrored.astype(jnp.float32))).astype(
        jnp.bfloat16
    )


MESH = pl.DeviceIdType.MESH
D = DILATION_STEP
BF = jnp.bfloat16
F32 = jnp.float32


def low_half():
    return lax.broadcasted_iota(jnp.int32, (1, 128), 1) < 64


def half_roll(v):
    return pltpu.roll(v, 64, 1)


def three_shifts(v):
    gap = jnp.zeros((D, v.shape[1]), v.dtype)
    left = jnp.concatenate([gap, v[:-D]], axis=0)
    right = jnp.concatenate([v[D:], gap], axis=0)
    return jnp.concatenate([left.astype(BF), v.astype(BF), right.astype(BF)], axis=1)


def times(a, w):
    return lax.dot_general(a, w, (((1,), (1,)), ((), ())), preferred_element_type=F32)


def fold_rows(v):
    return jnp.sum(v.reshape(v.shape[0] // 8, 8, v.shape[1]), axis=0)


def elu(v):
    return jnp.where(v > 0, v, jnp.exp(jnp.minimum(v, 0.0)) - 1.0)


def fused(
    n,
    pair_hbm, feats_hbm, w_row_hbm, w_col_hbm, taps1_hbm, taps2_hbm, scale_hbm, shift_hbm,
    out,
    feats, w_row, w_col, taps1, taps2, scale, shift,
    pair_up, pair_dn, halo_up, halo_dn, p32, h32, parts_own, parts_all, own_w, halo_w, col_conv, col_base, acc,
    edges, stats, block, tiles, mirror, m32, o32, out_v,
    in_sem, feat_s, feat_r, stat_s, stat_r, edge_s, edge_r, mir_s, mir_r, out_sem,
):
    me = lax.axis_index("gx")
    ch, _, cols = pair_up.shape
    rows = 2 * D
    half = n // 2
    side = lax.div(me, half)
    lane = lax.rem(me, half)
    cells = float(n * rows * cols)
    low = low_half()

    def peer_of(k):
        return lax.rem(side + 1 + lax.div(k, half), 2) * half + lax.rem(lane + k, half)

    def sender_of(k):
        return lax.rem(side + 1 + lax.div(k, half), 2) * half + lax.rem(lane + n - k, half)

    def far_peers(act):
        pl.loop(0, half)(act)

    def near_peers(act):
        pl.loop(half + 1, n)(act)

    def all_peers(act):
        far_peers(act)
        near_peers(act)

    barrier = pltpu.get_barrier_semaphore()

    @all_peers
    def _(k):
        pl.semaphore_signal(barrier, inc=1, device_id={"gx": peer_of(k)}, device_id_type=MESH)

    loads = [
        pltpu.make_async_copy(src, dst, in_sem.at[k])
        for k, (src, dst) in enumerate(
            (
                (feats_hbm, feats), (pair_hbm.at[:, pl.ds(0, D), :], pair_up),
                (pair_hbm.at[:, pl.ds(D, D), :], pair_dn), (w_row_hbm, w_row), (w_col_hbm, w_col),
                (taps1_hbm, taps1), (taps2_hbm, taps2), (scale_hbm, scale), (shift_hbm, shift),
            )
        )
    ]
    for load in loads:
        load.start()
    for load in loads[:5]:
        load.wait()

    def packed_rows(w):
        both = times(feats[...], jnp.concatenate([w[...]] * 2, axis=0))
        return jnp.where(low, both[:D], both[D:]).astype(BF)

    packed = jnp.concatenate([packed_rows(w_col), packed_rows(w_row)], axis=0)
    own_rows = packed[D:].astype(F32)
    parts_own[...] = packed
    parts_all[me] = packed
    pl.semaphore_wait(barrier, n - 1)

    def copy_to(src, dst, s, r, peer):
        return pltpu.make_async_remote_copy(
            src_ref=src, dst_ref=dst, send_sem=s, recv_sem=r,
            device_id={"gx": peer}, device_id_type=MESH,
        )

    def feat_copy(k):
        return copy_to(parts_own, parts_all.at[me], feat_s.at[k], feat_r.at[k], peer_of(k))

    def stat_copy(index, k):
        return copy_to(
            stats.at[index, me], stats.at[index, me], stat_s.at[index, k], stat_r.at[index, k],
            peer_of(k),
        )

    def mirror_copy(k):
        peer = peer_of(k)
        return copy_to(tiles.at[peer], mirror.at[me], mir_s.at[k], mir_r.at[k], peer)

    def edge_copies(index):
        above, below = jnp.maximum(me - 1, 0), jnp.minimum(me + 1, n - 1)
        s, r = edge_s.at[index], edge_r.at[index]
        if index == 0:
            return (
                copy_to(pair_up, halo_dn, s.at[0], r.at[0], above),
                copy_to(pair_dn, halo_up, s.at[1], r.at[1], below),
            )
        return (
            copy_to(edges.at[0], edges.at[3], s.at[0], r.at[0], above),
            copy_to(edges.at[1], edges.at[2], s.at[1], r.at[1], below),
        )

    def edges_start(index):
        first, second = edge_copies(index)

        @pl.when(me > 0)
        def _():
            first.start()

        @pl.when(me < n - 1)
        def _():
            second.start()

    def edges_wait_recv(index):
        first, second = edge_copies(index)

        @pl.when(me < n - 1)
        def _():
            first.wait_recv()

        @pl.when(me > 0)
        def _():
            second.wait_recv()

    def edges_wait_send(index):
        first, second = edge_copies(index)

        @pl.when(me > 0)
        def _():
            first.wait_send()

        @pl.when(me < n - 1)
        def _():
            second.wait_send()

    @all_peers
    def _(k):
        feat_copy(k).start()

    edges_start(0)

    for load in loads[5:]:
        load.wait()

    halves = cols // 128
    for h in range(halves):
        where = slice(h * 128, h * 128 + 128)
        p32[h, 0] = pair_up[:, :, where].astype(F32).reshape(ch * D, 128)
        p32[h, 1] = pair_dn[:, :, where].astype(F32).reshape(ch * D, 128)

    def pick(values, i):
        chosen = lax.broadcasted_iota(jnp.int32, values.shape, 0) == i
        return jnp.sum(jnp.where(chosen, values, 0.0), axis=0, keepdims=True)

    def with_rows(source, row_values, i):
        parts = []
        for h in range(halves):
            first = source[h, 0, pl.ds(i, ch, stride=D), :]
            second = source[h, 1, pl.ds(i, ch, stride=D), :]
            parts.append(jnp.concatenate([first, second], axis=0).T)
        return jnp.concatenate(parts, axis=0) + pick(row_values, i)

    def pack(i, early, late):
        edges[0, i] = jnp.where(low, early, half_roll(late)).astype(BF)
        edges[1, i] = jnp.where(low, half_roll(early), late).astype(BF)

    for index, taps in enumerate((taps1, taps2)):
        t = taps[...].astype(F32)
        none = jnp.zeros_like(t[0])
        for kx in range(3):
            where = slice(kx * 128, kx * 128 + 128)
            top = jnp.concatenate([t[3 + kx], t[6 + kx]], axis=1)
            bottom = jnp.concatenate([t[kx], t[3 + kx]], axis=1)
            own_w[index, :, where] = jnp.concatenate([top, bottom], axis=0).astype(BF)
            top = jnp.concatenate([t[kx], none], axis=1)
            bottom = jnp.concatenate([none, t[6 + kx]], axis=1)
            halo_w[index, :, where] = jnp.concatenate([top, bottom], axis=0).astype(BF)

    @pl.loop(0, D, unroll=D)
    def _(i):
        v = with_rows(p32, own_rows, i)
        block[i] = v.astype(BF)
        acc[i] = times(three_shifts(v), own_w[0])

    @all_peers
    def _(k):
        feat_copy(k).wait_recv()

    inside = jnp.where(low, (me > 0).astype(F32), (me < n - 1).astype(F32)) > 0.5
    part = parts_all[...].astype(F32)[:, :D].reshape(n * D, 128)
    swapped = half_roll(part)
    even = jnp.where(low, part, swapped).reshape(n, 1, D, 128)
    odd = jnp.where(low, swapped, part).reshape(n, 1, D, 128)
    col_part = jnp.concatenate([even, odd], axis=1).reshape(cols, 128)
    col_conv[...] = times(three_shifts(col_part), own_w[0]) + times(
        three_shifts(jnp.where(inside, col_part, 0.0)), halo_w[0]
    )
    col_base[...] = col_part + jnp.concatenate([shift[1:2, :]] * 2, axis=1)

    def unpacked(i):
        u = edges[2, i].astype(F32)
        d = edges[3, i].astype(F32)
        return jnp.where(low, u, half_roll(d)), jnp.where(low, half_roll(u), d)

    def add_sums(sums, a):
        return sums[0] + fold_rows(a), sums[1] + fold_rows(a * a)

    zeros = jnp.zeros((8, 128), F32)

    def publish(index, sums):
        lines = []
        for v in sums:
            v = jnp.sum(v, axis=0, keepdims=True)
            lines.append(v + half_roll(v))
        stats[index, me] = jnp.where(low, lines[0], lines[1])

        @all_peers
        def _(k):
            stat_copy(index, k).start()

    def collect(index):
        @all_peers
        def _(k):
            stat_copy(index, k).wait_recv()

        total = jnp.sum(stats[index], axis=0)
        swapped = half_roll(total)
        average = jnp.where(low, total, swapped) / cells
        spread = jnp.where(low, swapped, total) / cells - average * average
        gain = jnp.concatenate([scale[index : index + 1, :]] * 2, axis=1)
        return average, gain * lax.rsqrt(spread + epsilon)

    rows_up = parts_all[jnp.maximum(me - 1, 0)].astype(F32)[D:]
    rows_dn = parts_all[jnp.minimum(me + 1, n - 1)].astype(F32)[D:]
    halo_rows = half_roll(jnp.where(low, rows_dn, rows_up))

    edges_wait_recv(0)
    for h in range(halves):
        where = slice(h * 128, h * 128 + 128)
        h32[h, 0] = halo_up[:, :, where].astype(F32).reshape(ch * D, 128)
        h32[h, 1] = halo_dn[:, :, where].astype(F32).reshape(ch * D, 128)

    def first_edge(i, sums):
        results = []
        for offset in (0, D // 2):
            v = jnp.where(inside, with_rows(h32, halo_rows, i + offset), 0.0)
            a = acc[i + offset] + times(three_shifts(v), halo_w[0]) + col_conv[...]
            acc[i + offset] = a
            sums = add_sums(sums, a)
            results.append(a)
        pack(i, *results)
        return sums

    sums = lax.fori_loop(0, D // 2, first_edge, (zeros, zeros), unroll=D // 2)
    publish(0, sums)
    edges_start(1)
    average, factor = collect(0)
    base = jnp.concatenate([shift[0:1, :]] * 2, axis=1)

    @pl.loop(0, D, unroll=D)
    def _(i):
        a = elu((acc[i] - average) * factor + base)
        acc[i] = times(three_shifts(a), own_w[1])

    edges_wait_recv(1)

    def second_edge(i, sums):
        for offset, v in zip((0, D // 2), unpacked(i)):
            v = jnp.where(inside, elu((v - average) * factor + base), 0.0)
            a = acc[i + offset] + times(three_shifts(v), halo_w[1])
            acc[i + offset] = a
            sums = add_sums(sums, a)
        return sums

    sums = lax.fori_loop(0, D // 2, second_edge, (zeros, zeros), unroll=D // 2)
    publish(1, sums)
    average2, factor2 = collect(1)

    def result_of(which):
        where = pl.ds(pl.multiple_of(which * 128, 128), 128)

        @pl.loop(0, D, unroll=D)
        def _(i):
            v = block[i, where, :].astype(F32) + col_base[where, :]
            v = v + (acc[i, where, :] - average2) * factor2
            tiles[pl.ds(which * half, half), i] = elu(v).astype(BF).reshape(half, rows, 128)

    def widen(e):
        start = pl.multiple_of(e * (D * rows), D * rows)
        m32[pl.ds(start, D * rows), :] = mirror[e].astype(F32).reshape(D * rows, 128)

    def finish(which):
        where = pl.ds(pl.multiple_of(which * 128, 128), 128)
        offset = which * (half * D * rows)

        @pl.loop(0, D, unroll=D)
        def _(i):
            first = m32[pl.ds(offset + i, half * D, stride=rows), :]
            second = m32[pl.ds(offset + i + D, half * D, stride=rows), :]
            even = jnp.where(low, first, half_roll(second)).reshape(half, 1, D, 128)
            odd = jnp.where(low, half_roll(first), second).reshape(half, 1, D, 128)
            m = jnp.concatenate([even, odd], axis=1).reshape(128, 128)
            own = tiles[pl.ds(which * half, half), i].astype(F32).reshape(128, 128)
            t = (0.5 * (own + m)).T
            o32[which, pl.ds(i, ch, stride=rows), :] = t[:ch]
            o32[which, pl.ds(i + D, ch, stride=rows), :] = t[ch:]

        out_v[which] = o32[which].reshape(ch, rows, 128).astype(BF)
        copy = pltpu.make_async_copy(out_v.at[which], out.at[:, :, where], out_sem.at[which])
        copy.start()
        return copy

    result_of(1 - side)

    @far_peers
    def _(k):
        mirror_copy(k).start()

    result_of(side)

    @near_peers
    def _(k):
        mirror_copy(k).start()

    mirror[me] = tiles[me]
    widen(me)

    @near_peers
    def _(k):
        mirror_copy(k).wait_recv()
        widen(sender_of(k))

    near = finish(side)

    @all_peers
    def _(k):
        feat_copy(k).wait_send()
        stat_copy(0, k).wait_send()
        stat_copy(1, k).wait_send()

    edges_wait_send(0)
    edges_wait_send(1)

    @far_peers
    def _(k):
        mirror_copy(k).wait_recv()
        widen(sender_of(k))

    far = finish(1 - side)

    @all_peers
    def _(k):
        mirror_copy(k).wait_send()

    near.wait()
    far.wait()


def fused_body(n, *args):
    residue_feats, pair_feats = args[:2]
    ch, rows, cols = pair_feats.shape
    halves = cols // 128
    rest = (args[2].T, args[3].T) + args[4:]
    dma = pltpu.SemaphoreType.DMA
    return pl.pallas_call(
        functools.partial(fused, n),
        out_shape=jax.ShapeDtypeStruct(pair_feats.shape, BF),
        in_specs=[pl.BlockSpec(memory_space=pltpu.HBM)] * 8,
        out_specs=pl.BlockSpec(memory_space=pl.ANY),
        scratch_shapes=[
            *[pltpu.VMEM(a.shape, a.dtype) for a in (residue_feats,) + rest],
            *[pltpu.VMEM((ch, D, cols), BF)] * 4,
            *[pltpu.VMEM((halves, 2, ch * D, 128), F32)] * 2,
            pltpu.VMEM((rows, 128), BF),
            pltpu.VMEM((n, rows, 128), BF),
            pltpu.VMEM((2, 128, 384), BF),
            pltpu.VMEM((2, 128, 384), BF),
            pltpu.VMEM((cols, 128), F32),
            pltpu.VMEM((cols, 128), F32),
            pltpu.VMEM((D, cols, 128), F32),
            pltpu.VMEM((4, D // 2, cols, 128), BF),
            pltpu.VMEM((2, n, 1, 128), F32),
            pltpu.VMEM((D, cols, 128), BF),
            *[pltpu.VMEM((n, D, rows, 128), BF)] * 2,
            pltpu.VMEM((n * D * rows, 128), F32),
            pltpu.VMEM((halves, ch * rows, 128), F32),
            pltpu.VMEM((halves, ch, rows, 128), BF),
            dma((9,)),
            dma((n,)), dma((n,)), dma((2, n)), dma((2, n)), dma((2, 2)), dma((2, 2)),
            dma((n,)), dma((n,)), dma((2,)),
        ],
        compiler_params=pltpu.CompilerParams(
            collective_id=0, has_side_effects=True, vmem_limit_bytes=63 * 1024 * 1024
        ),
    )(pair_feats, residue_feats, *rest)


def solution(mesh):
    placed = (P(("grp", "gx"), None), P(None, ("grp", "gx"), "gy"), P(), P(), P(), P(), P(), P())
    n = mesh.shape["gx"]

    def chosen(*args):
        ch, rows, cols = args[1].shape
        fits = mesh.shape["gy"] == 1 and rows == 2 * D and cols == n * rows
        if fits and ch == 64 and cols == 256:
            return fused_body(n, *args)
        return body(*args)

    return jax.shard_map(
        chosen, mesh=mesh, in_specs=placed, out_specs=P(None, ("grp", "gx"), "gy"), check_vma=False
    )
```
